32 devices in a mesh: img: 2 (over x), ga: 4 (over y, core), band: 4 (over z).
Axes of the slice: x: 2, y: 2, z: 4, core: 2. Of those that a mesh axis runs over, the one named last changes fastest.
Arguments:
- orbitals: bfloat16 [1536, 12288], P(('img', 'band'), 'ga'), parts along dimension 0, as said below
- kernel: float32 [12288], P('ga'), may hold values from 0.3 to 3
- block_vectors: bfloat16 [512, 12288], P(('img', 'band'), 'ga'), parts along dimension 0
Outputs:
- ace_vectors: bfloat16 [1536, 12288], P(('img', 'band'), 'ga'), parts along dimension 0
- exchange_block: bfloat16 [512, 12288], P(('img', 'band'), 'ga'), parts along dimension 0
The draws below stay inside these ranges and needn't reach their ends.
There are 2 independent parts, one for each index of `img`. The reference program is written for one: setup_inputs(seed, part) draws one part's arguments, and reference() takes and returns one part's arrays. A program takes and returns all parts, laid end to end along the dimension named above; an argument that names none is the same for every part. Nothing has to cross between parts.
Inputs may be any that keep to these rules, and one draw needn't show every extreme that they name: `orbitals`: the bands of one image are linearly independent, and the block lies largely in their span.
All inputs are finite; a program needn't handle non-finite values.
Results may differ from the reference program's by a relative error of at most 0.02.
Values may be sent and summed in bfloat16 or wider, within the bound.
A program may use at most 64 MiB of HBM per device.

```python
import math
import jax
import jax.numpy as jnp
from jax import lax

NB = 768
NBLK = 256
NG = 12288


def orbital_pair(key):
    independent = jax.random.normal(jax.random.fold_in(key, 11), (NB, NG), jnp.float32)
    mixing = jax.random.normal(jax.random.fold_in(key, 12), (NB, NB), jnp.float32) * (0.4 / math.sqrt(NB))
    orbital_rows = independent + jnp.dot(mixing, independent, precision=lax.Precision.HIGHEST)
    mixture = jax.random.normal(jax.random.fold_in(key, 13), (NBLK, NB), jnp.float32) / math.sqrt(NB)
    residue = jax.random.normal(jax.random.fold_in(key, 14), (NBLK, NG), jnp.float32)
    block_rows = jnp.dot(mixture, orbital_rows, precision=lax.Precision.HIGHEST) + 0.5 * residue
    return (orbital_rows, block_rows)


def draw_orbitals(key, part):
    return orbital_pair(key)[0].astype(jnp.bfloat16)


def draw_block_vectors(key, part):
    return orbital_pair(key)[1].astype(jnp.bfloat16)


def steps_of(rng, extent, pieces, least, high):
    gain, own = 1.0, jax.random.fold_in(rng, 6)
    for position, blocks in pieces:
        heights = jnp.exp(jax.random.uniform(jax.random.fold_in(own, position), (blocks,), jnp.float32, least / len(pieces), high / len(pieces)))
        gain = gain * jnp.repeat(heights, extent[position] // blocks).reshape([-1 if axis == position else 1 for axis in range(len(extent))])
    return gain


def setup_inputs(seed: int = 0, part: int = 0) -> dict:
    arg_keys = jax.random.split(jax.random.key(seed), 4)
    part_keys = jax.random.split(jax.random.fold_in(arg_keys[3], part), 4)
    orbitals = draw_orbitals(jax.random.fold_in(jax.random.fold_in(arg_keys[3], part), 71), part)
    kernel = jnp.clip(jnp.exp(math.log(3.0) - 2.3025851 * jax.random.uniform(arg_keys[1], (NG,), jnp.float32) ** steps_of(arg_keys[1], (NG,), ((0, 4),), -0.2, 0.2)), 0.3, 3.0)
    block_vectors = draw_block_vectors(jax.random.fold_in(jax.random.fold_in(arg_keys[3], part), 71), part)
    return {"orbitals": orbitals, "kernel": kernel, "block_vectors": block_vectors}


def reference(orbitals, kernel, block_vectors):
    weighted = (-(orbitals.astype(jnp.float32) * kernel[None, :])).astype(jnp.bfloat16)
    margin = -lax.dot_general(orbitals.astype(jnp.float32), weighted.astype(jnp.float32), (((1,), (1,)), ((), ())), preferred_element_type=jnp.float32) / NG
    factor = jnp.linalg.cholesky(margin)
    projector = lax.linalg.triangular_solve(factor, weighted.astype(jnp.float32), left_side=True, lower=True)
    coupling = jnp.dot(projector, block_vectors.astype(jnp.float32).T, precision=lax.Precision.HIGHEST) / NG
    applied = -lax.dot_general(coupling, projector, (((0,), (0,)), ((), ())), precision=lax.Precision.HIGHEST)
    return (projector.astype(jnp.bfloat16), applied.astype(jnp.bfloat16))
```

```python
import functools

import jax
import jax.numpy as jnp
from jax import lax
from jax.experimental import pallas as pl
from jax.experimental.pallas import tpu as pltpu
from jax.sharding import PartitionSpec as P

MESH = pl.DeviceIdType.MESH
F32 = jnp.float32
BF16 = jnp.bfloat16
TILE = 128


def remote(src, dst, send_sem, recv_sem, where):
    return pltpu.make_async_remote_copy(
        src_ref=src, dst_ref=dst, send_sem=send_sem, recv_sem=recv_sem,
        device_id=where, device_id_type=MESH,
    )


def greet(places):
    barrier = pltpu.get_barrier_semaphore()
    for place in places:
        pl.semaphore_signal(barrier, inc=1, device_id=place, device_id_type=MESH)
    pl.semaphore_wait(barrier, len(places))


def dot(a, b, dims):
    return lax.dot_general(a, b, (dims, ((), ())), preferred_element_type=F32)


class Place:
    def __init__(self, bands, groups):
        self.bands = bands
        self.me = lax.axis_index("band")
        self.team = bands // 2
        self.half = self.me // self.team
        self.rank = lax.rem(self.me, self.team)
        ga = lax.axis_index("ga")
        self.core = lax.rem(ga, 2)
        self.row = lax.rem(ga // 2, 2)
        self.partner = {"ga": ga + 1 - 2 * self.core}
        self.across = {"ga": ga + 2 - 4 * self.row}
        self.peer = [lax.rem(self.me + d, bands) for d in range(bands)]
        self.far = sorted(range(1, bands), key=lambda d: -min(d, bands - d))
        self.near = self.far[::-1]
        self.bits = []
        stride = 4
        while stride < groups:
            self.bits.append({"ga": ga + stride * (1 - 2 * lax.rem(ga // stride, 2))})
            stride *= 2

    def band(self, d):
        return {"band": self.peer[d]}

    def mate(self, j):
        return lax.rem(self.rank + j, self.team)

    def rival(self, t):
        return (1 - self.half) * (self.team + t) + self.half * (self.team - 1 - t)

    def everyone(self):
        return [self.band(d) for d in range(1, self.bands)] + [self.partner, self.across] + self.bits


def span(index, size, offset=0, stride=None):
    return pl.ds(pl.multiple_of(offset + index * (stride or size), 16), size)


def reduce_scratch(rows, parts, bands, levels, sides):
    h1, h2 = rows // 2, rows // 4
    h3 = h2 // parts
    dma = pltpu.SemaphoreType.DMA
    shapes = [
        ((rows, TILE), F32), ((rows, TILE), BF16), ((h1, TILE), BF16),
        ((h1, TILE), F32), ((h1, TILE), BF16), ((h2, TILE), BF16),
        ((h2, TILE), F32), ((h2, TILE), BF16), ((parts, h3, TILE), BF16),
        ((levels, h3, TILE), BF16), ((levels, h3, TILE), BF16), ((sides * rows, TILE), BF16),
    ]
    return [pltpu.VMEM(*shape) for shape in shapes] + [
        dma((4,)), dma((parts,)), dma((parts,)), dma((levels,)), dma((levels,)),
        dma((bands,)), dma((bands,)), dma((bands,)), dma((bands,)),
        dma((2 * bands,)), dma((2 * bands,)),
    ]


SCRATCH = 23


class Reduce:
    def __init__(self, at, scratch, by_team):
        self.at = at
        (self.p32, self.p16, self.rx1, self.a32, self.a16, self.rx2, self.b32, self.b16, self.rx3,
         self.out_x, self.rx_x, self.allg, self.one, self.z_s, self.z_r, self.x_s, self.x_r,
         self.g_s, self.g_r, self.y_s, self.y_r, self.f_s, self.f_r) = scratch
        self.rows = self.p32.shape[0]
        self.h1, self.h2, self.h3 = self.rx1.shape[0], self.rx2.shape[0], self.rx3.shape[1]
        self.by_team = by_team
        if by_team:
            self.mine = at.rank
            self.parts = [(j, at.mate(j), {"band": at.half * at.team + at.mate(j)})
                          for j in range(1, at.team)]
        else:
            self.mine = at.me
            self.parts = [(d, at.peer[d], at.band(d)) for d in at.far]

    def put(self, row, value):
        size = value.shape[0]
        self.p32[row:row + size, :] = value
        self.p16[row:row + size, :] = value.astype(BF16)

    def pad(self, row):
        size = self.rows - row
        if size:
            self.put(row, jnp.zeros((size, TILE), F32))

    def to_partner(self):
        at = self.at
        return remote(self.p16.at[span(1 - at.core, self.h1)], self.rx1,
                      self.one.at[0], self.one.at[1], at.partner)

    def to_across(self):
        at = self.at
        return remote(self.a16.at[span(1 - at.row, self.h2)], self.rx2,
                      self.one.at[2], self.one.at[3], at.across)

    def to_parts(self):
        return [remote(self.b16.at[span(index, self.h3)], self.rx3.at[slot],
                       self.z_s.at[slot], self.z_r.at[slot], where)
                for slot, index, where in self.parts]

    def piece(self, d, row):
        at = self.at
        source = lax.rem(at.me + at.bands - d, at.bands)
        offset = at.core * self.h1 + row * self.h2
        if self.by_team:
            offset = offset + (source // at.team) * self.rows
            source = lax.rem(source, at.team)
        return span(source, self.h3, offset)

    def gather(self, d):
        own = self.allg.at[self.piece(0, self.at.row)]
        return remote(own, own, self.g_s.at[d], self.g_r.at[d], self.at.band(d))

    def side(self, d):
        there = self.allg.at[self.piece(d, self.at.row)]
        return remote(there, there, self.y_s.at[d], self.y_r.at[d], self.at.across)

    def last(self, d, other):
        row = 1 - self.at.row if other else self.at.row
        there = self.allg.at[self.piece(d, row)]
        e = d + self.at.bands * other
        return remote(there, there, self.f_s.at[e], self.f_r.at[e], self.at.partner)

    def s1(self):
        self.to_partner().start()

    def s2(self):
        self.to_partner().wait()
        self.a32[...] = self.p32[span(self.at.core, self.h1), :] + self.rx1[...].astype(F32)
        self.a16[...] = self.a32[...].astype(BF16)
        self.to_across().start()

    def s3(self):
        self.to_across().wait()
        self.b32[...] = self.a32[span(self.at.row, self.h2), :] + self.rx2[...].astype(F32)
        self.b16[...] = self.b32[...].astype(BF16)
        for copy in self.to_parts():
            copy.start()

    def s4(self):
        at = self.at
        for copy in self.to_parts():
            copy.wait()
        total = self.b32[span(self.mine, self.h3), :]
        for slot, _, _ in self.parts:
            total = total + self.rx3[slot].astype(F32)
        for i, place in enumerate(at.bits):
            self.out_x[i] = total.astype(BF16)
            copy = remote(self.out_x.at[i], self.rx_x.at[i], self.x_s.at[i], self.x_r.at[i], place)
            copy.start()
            copy.wait()
            total = self.out_x[i].astype(F32) + self.rx_x[i].astype(F32)
        self.allg[self.piece(0, at.row), :] = total.astype(BF16)
        for d in at.far:
            self.gather(d).start()
        self.side(0).start()
        self.last(0, 0).start()

    def s5(self):
        for d in self.at.near:
            self.gather(d).wait()
            self.side(d).start()
            self.last(d, 0).start()

    def s6(self):
        for d in [0] + self.at.near:
            self.side(d).wait()
            self.last(d, 1).start()

    def s7(self):
        for d in [0] + self.at.near:
            self.last(d, 0).wait()
            self.last(d, 1).wait()


def split(a):
    high = a.astype(BF16)
    return high, (a - high.astype(F32)).astype(BF16)


def product3(a, b, dims):
    (ah, al), (bh, bl) = split(a), split(b)
    return dot(ah, bh, dims) + (dot(ah, bl, dims) + dot(al, bh, dims))


def identity(rows):
    shape = (rows, rows)
    return (lax.broadcasted_iota(jnp.int32, shape, 0)
            == lax.broadcasted_iota(jnp.int32, shape, 1)).astype(F32)


def factor_tile(d_ref, t_ref, hooks):
    G, SUB, BLK = 32, 8, 16
    H, K = G // SUB, BLK // SUB
    sub = lax.broadcasted_iota(jnp.int32, (SUB, TILE), 0)

    def spread(block, i):
        return jnp.broadcast_to(block[i:i + 1, :], (SUB, TILE))

    def lane(block, c):
        where = jnp.broadcast_to(c, (SUB, TILE))
        return jnp.take_along_axis(block, where, axis=1, mode="promise_in_bounds")

    def step(g, carry):
        start = pl.multiple_of(g * G, G)
        lefts = [d_ref[pl.ds(start + h * SUB, SUB), 0:TILE] for h in range(H)]
        rights = [d_ref[pl.ds(start + h * SUB, SUB), TILE:2 * TILE] for h in range(H)]
        us, vs = [], []
        for b in range(G // BLK):
            h0 = b * K
            cols = [{h: lane(lefts[h], start + (b * BLK + c)) for h in range(h0 + c // SUB, H)}
                    for c in range(BLK)]
            low = [[None] * BLK for _ in range(BLK)]
            u, v = [], []
            u_rows = [jnp.zeros((SUB, TILE), F32) for _ in range(K)]
            v_rows = [jnp.zeros((SUB, TILE), F32) for _ in range(K)]
            for j in range(BLK):
                k, i = j // SUB, j % SUB
                r = lax.rsqrt(spread(cols[j][h0 + k], i))
                for h in range(h0 + k, H):
                    cols[j][h] = cols[j][h] * r
                for c in range(j + 1, BLK):
                    low[c][j] = spread(cols[j][h0 + c // SUB], c % SUB)
                    for h in range(h0 + c // SUB, H):
                        cols[c][h] = cols[c][h] - cols[j][h] * low[c][j]
                p, q = spread(lefts[h0 + k], i), spread(rights[h0 + k], i)
                for t in range(j):
                    p = p - low[j][t] * u[t]
                    q = q - low[j][t] * v[t]
                u.append(p * r)
                v.append(q * r)
                u_rows[k] = jnp.where(sub == i, u[j], u_rows[k])
                v_rows[k] = jnp.where(sub == i, v[j], v_rows[k])
            us += u_rows
            vs += v_rows
            for h in range(h0 + K, H):
                for j in range(BLK):
                    lefts[h] = lefts[h] - cols[j][h] * u[j]
                    rights[h] = rights[h] - cols[j][h] * v[j]
        u_all = jnp.concatenate(us, axis=0)
        v_all = jnp.concatenate(vs, axis=0)
        t_ref[pl.ds(start, G), :] = v_all
        both = jnp.concatenate([u_all, v_all], axis=1)
        high = both.astype(BF16).astype(F32)
        low = both - high
        lhs = jnp.concatenate([high[:, :TILE], high[:, :TILE], low[:, :TILE]], axis=0)
        rhs = jnp.concatenate([high, low, high], axis=0)
        d_ref[...] -= dot(lhs.astype(BF16), rhs.astype(BF16), ((0,), (0,)))
        for k, hook in enumerate(hooks):
            if hook is not None:
                pl.when(g == k)(hook)
        return carry

    lax.fori_loop(0, TILE // G, step, 0)


def ace_kernel(bands, groups, orb, kern, blk, ace, exch, full, extra, w, wx, a, rest, x16, xlow, mba,
               d_ref, t_ref, proj, bfull, acc, applied, loc, m_s, m_r, n_s, n_r, c_s, c_r,
               b_s, b_r, p_s, p_r, e_s, e_r, *scratch):
    at = Place(bands, groups)
    me, team = at.me, at.team
    own, bown = ace.shape[0], exch.shape[0]
    cols = w.shape[1]
    n, nblk = own * bands, bown * bands
    n2 = n // 2
    scale = 1.0 / (ace.shape[1] * groups)
    inner = Reduce(at, scratch[:SCRATCH], True)
    cross = Reduce(at, scratch[SCRATCH:2 * SCRATCH], False)
    couple = Reduce(at, scratch[2 * SCRATCH:], False)
    greet(at.everyone())

    def chunk(index):
        return pl.ds(pl.multiple_of(index * cols, TILE), cols)

    def twin(index):
        return chunk(lax.rem(index + team, bands))

    mine = full.at[span(me, own)]
    also = extra.at[span(at.rank, own)]
    bmine = bfull.at[span(me, bown)]

    def kept():
        return [pltpu.make_async_copy(orb.at[:, chunk(me)], mine, loc.at[0]),
                pltpu.make_async_copy(orb.at[:, twin(me)], also, loc.at[1])]

    def to_mates():
        copies = []
        for j in range(1, team):
            p = at.half * team + at.mate(j)
            copies.append(remote(orb.at[:, chunk(p)], mine, m_s.at[j], m_r.at[j], {"band": p}))
            copies.append(remote(orb.at[:, twin(p)], also, n_s.at[j], n_r.at[j], {"band": p}))
        return copies

    def to_rival(t, sender):
        p = at.rival(t)
        return remote(orb.at[:, chunk(p)], mine, c_s.at[t], c_r.at[sender], {"band": p})

    def blocks():
        return [remote(blk.at[:, chunk(at.peer[d])], bmine, b_s.at[d], b_r.at[d], at.band(d))
                for d in at.far]

    def bkept():
        return pltpu.make_async_copy(blk.at[:, chunk(me)], bmine, loc.at[2])

    for copy in to_mates():
        copy.start()
    for t in range(team):
        to_rival(t, at.rank).start()
    for copy in kept():
        copy.start()
    bkept().start()

    def weigh(rows, columns):
        return (-(rows.astype(F32) * kern[:, columns])).astype(BF16)

    for copy in kept() + to_mates():
        copy.wait()
    band = span(at.half, n2)
    w[band, :] = weigh(full[band, :], chunk(me))
    wx[...] = weigh(extra[...], twin(me))
    row = 0
    for s in range(0, n2, TILE):
        e = s + TILE
        product = (dot(w[span(at.half, TILE, s, n2), :], full[span(at.half, e, 0, n2), :],
                       ((1,), (1,)))
                   + dot(wx[s:e, :], extra[0:e, :], ((1,), (1,))))
        for c in range(0, e, TILE):
            inner.put(row, product[:, c:c + TILE])
            row += TILE
    inner.pad(row)
    inner.s1()
    inner.s2()
    inner.s3()
    inner.s4()
    for copy in blocks():
        copy.start()
    for t in range(team):
        to_rival(t, t).wait_recv()
    other = span(1 - at.half, n2)
    w[other, :] = weigh(full[other, :], chunk(me))
    row = 0
    for s in range(n2, n, TILE):
        product = dot(w[s:s + TILE, :], full[0:n2, :], ((1,), (1,)))
        for c in range(0, n2, TILE):
            cross.put(row, product[:, c:c + TILE])
            row += TILE
    cross.pad(row)
    cross.s1()
    inner.s5()
    cross.s2()
    inner.s6()
    inner.s7()
    row = 0
    for base in (0, n2):
        for s in range(base, base + n2, TILE):
            for c in range(base, s + TILE, TILE):
                a[s:s + TILE, c:c + TILE] = inner.allg[row:row + TILE, :].astype(F32) * -scale
                row += TILE
        row = inner.rows
    rest[...] = identity(n)
    x16[...] = jnp.zeros_like(x16)

    def couple_start():
        bkept().wait()
        for copy in blocks():
            copy.wait()
        half = nblk // 2
        for h in range(2):
            couple.put(h * n, dot(w[...], bfull[h * half:(h + 1) * half, :], ((1,), (1,))))
        couple.s1()

    cuts = sorted(set(range(0, n, TILE)) | set(range(0, n, own)) | {n})
    pieces = list(enumerate(zip(cuts[:-1], cuts[1:])))

    def piece(q, r0, r1, source, target):
        lo = r0 % own
        return remote(proj.at[r0:r1], ace.at[lo:lo + r1 - r0, chunk(source)],
                      p_s.at[q], p_r.at[q, source], {"band": target})

    def stay(q, r0, r1):
        lo = r0 % own
        return pltpu.make_async_copy(
            proj.at[r0:r1], ace.at[lo:lo + r1 - r0, chunk(me)], p_s.at[q])

    def deliver(lo, hi):
        for q, (r0, r1) in pieces:
            if lo <= r0 < hi:
                owner = r0 // own

                @pl.when(me != owner)
                def _():
                    piece(q, r0, r1, me, owner).start()

                @pl.when(me == owner)
                def _():
                    stay(q, r0, r1).start()

    tiles = n2 // TILE
    first = [cross.s3, couple_start, cross.s4, couple.s2, cross.s5, couple.s3, cross.s6]
    slots = [(0, 1), (1, 0), (1, 1), (1, 2), (2, 0), (2, 1), (2, 2)]
    hooks = [[None] * 4 for _ in range(2 * tiles)]
    for (k, g), stage in zip(slots, first):
        hooks[min(k, tiles - 1)][g] = stage
    hooks[tiles][0], hooks[tiles][1], hooks[tiles][3] = couple.s5, couple.s6, couple.s7

    def attach(lo, hi):
        half = nblk // 2
        for h in range(2):
            part = allg_dot(lo, hi, h) * scale
            update = dot(part.astype(BF16), proj[lo:hi, :], ((0,), (0,)))
            if lo == 0:
                acc[h * half:(h + 1) * half, :] = update
            else:
                acc[h * half:(h + 1) * half, :] += update

    def allg_dot(lo, hi, h):
        return dot(x16[lo:hi, 0:hi], couple.allg[h * n:h * n + hi, :], ((1,), (0,)))

    for k, s in enumerate(range(0, n, TILE)):
        e = s + TILE
        top = n2 if s < n2 else n
        d_ref[:, 0:TILE] = a[s:e, s:e]
        d_ref[:, TILE:] = identity(TILE)
        factor_tile(d_ref, t_ref, hooks[k])
        tile = t_ref[...]
        rows = product3(tile, rest[s:e, 0:e], ((1,), (0,)))
        high, low = split(rows)
        x16[s:e, 0:e] = high
        if s < n2:
            xlow[s:e, 0:n2] = jnp.zeros((TILE, n2), BF16)
            xlow[s:e, 0:e] = low
        proj[s:e, :] = (dot(high, w[0:e, :], ((1,), (0,)))
                        + dot(low, w[0:e, :], ((1,), (0,)))).astype(BF16)
        if s >= n2:
            deliver(s, e)
        if e < top:
            panel = product3(a[e:top, s:e], tile, ((1,), (1,)))
            for c in range(e, top, TILE):
                a[c:top, c:c + TILE] -= product3(panel[c - e:], panel[c - e:c - s], ((1,), (1,)))
            rest[e:top, 0:e] -= product3(panel, rows, ((1,), (0,)))
        if e == n2:
            cross.s7()
            row = 0
            for r in range(0, n2, TILE):
                for c in range(0, n2, TILE):
                    mba[r:r + TILE, c:c + TILE] = cross.allg[row:row + TILE, :]
                    row += TILE
            both = (((1,), (1,)))
            below = (dot(mba[...], x16[0:n2, 0:n2], both) + dot(mba[...], xlow[...], both)) * -scale
            bh, bl = split(below)
            for c in range(0, n2, TILE):
                d = c + TILE
                a[n2 + c:n, n2 + c:n2 + d] -= (
                    dot(bh[c:], bh[c:d], both) + (dot(bh[c:], bl[c:d], both) + dot(bl[c:], bh[c:d], both)))
            over = ((1,), (0,))
            xh = x16[0:n2, 0:n2]
            rest[n2:, 0:n2] = -(dot(bh, xh, over) + (dot(bh, xlow[...], over) + dot(bl, xh, over)))
            couple.s4()
            deliver(0, n2)
        if e == n - TILE:
            attach(0, e)
    attach(n - TILE, n)
    applied[...] = (-acc[...]).astype(BF16)
    outs = [remote(applied.at[span(at.peer[d], bown)], exch.at[:, chunk(me)],
                   e_s.at[d], e_r.at[d], at.band(d)) for d in at.far]
    outs.append(pltpu.make_async_copy(applied.at[span(me, bown)], exch.at[:, chunk(me)], loc.at[3]))
    for copy in outs:
        copy.start()
    for t in range(team):
        to_rival(t, t).wait_send()
    for q, (r0, r1) in pieces:
        owner = r0 // own

        @pl.when(me != owner)
        def _():
            piece(q, r0, r1, me, owner).wait_send()

        @pl.when(me == owner)
        def _():
            stay(q, r0, r1).wait()
            for d in range(1, bands):
                piece(q, r0, r1, at.peer[d], at.peer[d]).wait_recv()
    for copy in outs:
        copy.wait()


def shards(orbitals, kernel, block_vectors):
    groups, bands = lax.axis_size("ga"), lax.axis_size("band")
    own, width = orbitals.shape
    bown = block_vectors.shape[0]
    cols = width // bands
    n, nblk = own * bands, bown * bands
    n2, team = n // 2, bands // 2
    levels = max(groups.bit_length() - 3, 1)
    tiles = n2 // TILE

    def padded(rows, parts):
        unit = 4 * parts * 16
        return -(-rows // unit) * unit

    pieces = len(set(range(0, n, TILE)) | set(range(0, n, own)))
    vmem, hbm = pl.BlockSpec(memory_space=pltpu.VMEM), pl.BlockSpec(memory_space=pl.ANY)
    dma = pltpu.SemaphoreType.DMA
    many, some = dma((bands,)), dma((team,))
    return pl.pallas_call(
        functools.partial(ace_kernel, bands, groups),
        name="ace",
        out_shape=(
            jax.ShapeDtypeStruct((own, width), BF16),
            jax.ShapeDtypeStruct((bown, width), BF16),
        ),
        in_specs=[hbm, vmem, hbm],
        out_specs=(hbm, hbm),
        scratch_shapes=[
            pltpu.VMEM((n, cols), BF16),
            pltpu.VMEM((n2, cols), BF16),
            pltpu.VMEM((n, cols), BF16),
            pltpu.VMEM((n2, cols), BF16),
            pltpu.VMEM((n, n), F32),
            pltpu.VMEM((n, n), F32),
            pltpu.VMEM((n, n), BF16),
            pltpu.VMEM((n2, n2), BF16),
            pltpu.VMEM((n2, n2), BF16),
            pltpu.VMEM((TILE, 2 * TILE), F32),
            pltpu.VMEM((TILE, TILE), F32),
            pltpu.VMEM((n, cols), BF16),
            pltpu.VMEM((nblk, cols), BF16),
            pltpu.VMEM((nblk, cols), F32),
            pltpu.VMEM((nblk, cols), BF16),
            dma((4,)), some, some, some, some, some, some,
            many, many, dma((pieces,)), dma((pieces, bands)), many, many,
        ]
        + reduce_scratch(padded(tiles * (tiles + 1) // 2 * TILE, team), team, bands, levels, 2)
        + reduce_scratch(padded(tiles * tiles * TILE, bands), bands, bands, levels, 1)
        + reduce_scratch(2 * n, bands, bands, levels, 1),
        compiler_params=pltpu.CompilerParams(
            collective_id=0, has_side_effects=True, vmem_limit_bytes=56 * 2**20),
    )(orbitals, kernel.reshape(1, width), block_vectors)


def solution(mesh):
    placed = (P(("img", "band"), "ga"), P("ga"), P(("img", "band"), "ga"))
    return jax.shard_map(
        shards,
        mesh=mesh,
        in_specs=placed,
        out_specs=(P(("img", "band"), "ga"), P(("img", "band"), "ga")),
        check_vma=False,
    )
```

```python
import functools

import jax
import jax.numpy as jnp
from jax import lax
from jax.experimental import pallas as pl
from jax.experimental.pallas import tpu as pltpu
from jax.sharding import PartitionSpec as P

MESH = pl.DeviceIdType.MESH
F32 = jnp.float32
BF16 = jnp.bfloat16
TILE = 128
SLICE = 16


def remote(src, dst, send_sem, recv_sem, where):
    return pltpu.make_async_remote_copy(
        src_ref=src, dst_ref=dst, send_sem=send_sem, recv_sem=recv_sem,
        device_id=where, device_id_type=MESH,
    )


def greet(places):
    barrier = pltpu.get_barrier_semaphore()
    for place in places:
        pl.semaphore_signal(barrier, inc=1, device_id=place, device_id_type=MESH)
    pl.semaphore_wait(barrier, len(places))


def dot(a, b, dims):
    return lax.dot_general(a, b, (dims, ((), ())), preferred_element_type=F32)


class Place:
    def __init__(self, bands, groups):
        self.bands = bands
        self.me = lax.axis_index("band")
        self.team = bands // 2
        self.half = self.me // self.team
        self.rank = lax.rem(self.me, self.team)
        ga = lax.axis_index("ga")
        self.core = lax.rem(ga, 2)
        self.row = lax.rem(ga // 2, 2)
        self.partner = {"ga": ga + 1 - 2 * self.core}
        self.across = {"ga": ga + 2 - 4 * self.row}
        self.peer = [lax.rem(self.me + d, bands) for d in range(bands)]
        self.far = sorted(range(1, bands), key=lambda d: -min(d, bands - d))
        self.near = self.far[::-1]
        self.bits = []
        stride = 4
        while stride < groups:
            self.bits.append({"ga": ga + stride * (1 - 2 * lax.rem(ga // stride, 2))})
            stride *= 2

    def band(self, d):
        return {"band": self.peer[d]}

    def mate(self, j):
        return lax.rem(self.rank + j, self.team)

    def rival(self, t):
        return (1 - self.half) * (self.team + t) + self.half * (self.team - 1 - t)

    def everyone(self):
        return [self.band(d) for d in range(1, self.bands)] + [self.partner, self.across] + self.bits


def span(index, size, offset=0, stride=None):
    return pl.ds(pl.multiple_of(offset + index * (stride or size), 16), size)


def reduce_scratch(rows, parts, bands, levels, sides):
    h1, h2 = rows // 2, rows // 4
    h3 = h2 // parts
    dma = pltpu.SemaphoreType.DMA
    shapes = [
        ((rows, TILE), F32), ((rows, TILE), BF16), ((h1, TILE), BF16),
        ((h1, TILE), F32), ((h1, TILE), BF16), ((h2, TILE), BF16),
        ((h2, TILE), F32), ((h2, TILE), BF16), ((parts, h3, TILE), BF16),
        ((levels, h3, TILE), BF16), ((levels, h3, TILE), BF16), ((sides * rows, TILE), BF16),
    ]
    return [pltpu.VMEM(*shape) for shape in shapes] + [
        dma((4,)), dma((parts,)), dma((parts,)), dma((levels,)), dma((levels,)),
        dma((bands,)), dma((bands,)), dma((bands,)), dma((bands,)),
        dma((2 * bands,)), dma((2 * bands,)),
    ]


SCRATCH = 23


class Reduce:
    def __init__(self, at, scratch, by_team):
        self.at = at
        (self.p32, self.p16, self.rx1, self.a32, self.a16, self.rx2, self.b32, self.b16, self.rx3,
         self.out_x, self.rx_x, self.allg, self.one, self.z_s, self.z_r, self.x_s, self.x_r,
         self.g_s, self.g_r, self.y_s, self.y_r, self.f_s, self.f_r) = scratch
        self.rows = self.p32.shape[0]
        self.h1, self.h2, self.h3 = self.rx1.shape[0], self.rx2.shape[0], self.rx3.shape[1]
        self.by_team = by_team
        if by_team:
            self.mine = at.rank
            self.parts = [(j, at.mate(j), {"band": at.half * at.team + at.mate(j)})
                          for j in range(1, at.team)]
        else:
            self.mine = at.me
            self.parts = [(d, at.peer[d], at.band(d)) for d in at.far]

    def put(self, row, value):
        size = value.shape[0]
        self.p32[row:row + size, :] = value
        self.p16[row:row + size, :] = value.astype(BF16)

    def pad(self, row):
        size = self.rows - row
        if size:
            self.put(row, jnp.zeros((size, TILE), F32))

    def to_partner(self):
        at = self.at
        return remote(self.p16.at[span(1 - at.core, self.h1)], self.rx1,
                      self.one.at[0], self.one.at[1], at.partner)

    def to_across(self):
        at = self.at
        return remote(self.a16.at[span(1 - at.row, self.h2)], self.rx2,
                      self.one.at[2], self.one.at[3], at.across)

    def to_parts(self):
        return [remote(self.b16.at[span(index, self.h3)], self.rx3.at[slot],
                       self.z_s.at[slot], self.z_r.at[slot], where)
                for slot, index, where in self.parts]

    def piece(self, d, row):
        at = self.at
        source = lax.rem(at.me + at.bands - d, at.bands)
        offset = at.core * self.h1 + row * self.h2
        if self.by_team:
            offset = offset + (source // at.team) * self.rows
            source = lax.rem(source, at.team)
        return span(source, self.h3, offset)

    def gather(self, d):
        own = self.allg.at[self.piece(0, self.at.row)]
        return remote(own, own, self.g_s.at[d], self.g_r.at[d], self.at.band(d))

    def side(self, d):
        there = self.allg.at[self.piece(d, self.at.row)]
        return remote(there, there, self.y_s.at[d], self.y_r.at[d], self.at.across)

    def last(self, d, other):
        row = 1 - self.at.row if other else self.at.row
        there = self.allg.at[self.piece(d, row)]
        e = d + self.at.bands * other
        return remote(there, there, self.f_s.at[e], self.f_r.at[e], self.at.partner)

    def s1(self):
        self.to_partner().start()

    def s2(self):
        self.to_partner().wait()
        self.a32[...] = self.p32[span(self.at.core, self.h1), :] + self.rx1[...].astype(F32)
        self.a16[...] = self.a32[...].astype(BF16)
        self.to_across().start()

    def s3(self):
        self.to_across().wait()
        self.b32[...] = self.a32[span(self.at.row, self.h2), :] + self.rx2[...].astype(F32)
        self.b16[...] = self.b32[...].astype(BF16)
        for copy in self.to_parts():
            copy.start()

    def s4(self):
        at = self.at
        for copy in self.to_parts():
            copy.wait()
        total = self.b32[span(self.mine, self.h3), :]
        for slot, _, _ in self.parts:
            total = total + self.rx3[slot].astype(F32)
        for i, place in enumerate(at.bits):
            self.out_x[i] = total.astype(BF16)
            copy = remote(self.out_x.at[i], self.rx_x.at[i], self.x_s.at[i], self.x_r.at[i], place)
            copy.start()
            copy.wait()
            total = self.out_x[i].astype(F32) + self.rx_x[i].astype(F32)
        self.allg[self.piece(0, at.row), :] = total.astype(BF16)
        for d in at.far:
            self.gather(d).start()
        self.side(0).start()
        self.last(0, 0).start()

    def s5(self):
        for d in self.at.near:
            self.gather(d).wait()
            self.side(d).start()
            self.last(d, 0).start()

    def s6(self):
        for d in [0] + self.at.near:
            self.side(d).wait()
            self.last(d, 1).start()

    def s7(self):
        for d in [0] + self.at.near:
            self.last(d, 0).wait()
            self.last(d, 1).wait()


def split(a):
    high = a.astype(BF16)
    return high, (a - high.astype(F32)).astype(BF16)


def product3(a, b, dims):
    (ah, al), (bh, bl) = split(a), split(b)
    return dot(ah, bh, dims) + (dot(ah, bl, dims) + dot(al, bh, dims))


def identity(rows):
    shape = (rows, rows)
    return (lax.broadcasted_iota(jnp.int32, shape, 0)
            == lax.broadcasted_iota(jnp.int32, shape, 1)).astype(F32)


def factor_tile(d_ref, t_ref, hooks):
    G, SUB, BLK = 32, 8, 16
    H, K = G // SUB, BLK // SUB
    sub = lax.broadcasted_iota(jnp.int32, (SUB, TILE), 0)

    def spread(block, i):
        return jnp.broadcast_to(block[i:i + 1, :], (SUB, TILE))

    def lane(block, c):
        where = jnp.broadcast_to(c, (SUB, TILE))
        return jnp.take_along_axis(block, where, axis=1, mode="promise_in_bounds")

    def step(g, carry):
        start = pl.multiple_of(g * G, G)
        lefts = [d_ref[pl.ds(start + h * SUB, SUB), 0:TILE] for h in range(H)]
        rights = [d_ref[pl.ds(start + h * SUB, SUB), TILE:2 * TILE] for h in range(H)]
        us, vs = [], []
        for b in range(G // BLK):
            h0 = b * K
            cols = [{h: lane(lefts[h], start + (b * BLK + c)) for h in range(h0 + c // SUB, H)}
                    for c in range(BLK)]
            low = [[None] * BLK for _ in range(BLK)]
            u, v = [], []
            u_rows = [jnp.zeros((SUB, TILE), F32) for _ in range(K)]
            v_rows = [jnp.zeros((SUB, TILE), F32) for _ in range(K)]
            for j in range(BLK):
                k, i = j // SUB, j % SUB
                r = lax.rsqrt(spread(cols[j][h0 + k], i))
                for h in range(h0 + k, H):
                    cols[j][h] = cols[j][h] * r
                for c in range(j + 1, BLK):
                    low[c][j] = spread(cols[j][h0 + c // SUB], c % SUB)
                    for h in range(h0 + c // SUB, H):
                        cols[c][h] = cols[c][h] - cols[j][h] * low[c][j]
                p, q = spread(lefts[h0 + k], i), spread(rights[h0 + k], i)
                for t in range(j):
                    p = p - low[j][t] * u[t]
                    q = q - low[j][t] * v[t]
                u.append(p * r)
                v.append(q * r)
                u_rows[k] = jnp.where(sub == i, u[j], u_rows[k])
                v_rows[k] = jnp.where(sub == i, v[j], v_rows[k])
            us += u_rows
            vs += v_rows
            for h in range(h0 + K, H):
                for j in range(BLK):
                    lefts[h] = lefts[h] - cols[j][h] * u[j]
                    rights[h] = rights[h] - cols[j][h] * v[j]
        u_all = jnp.concatenate(us, axis=0)
        v_all = jnp.concatenate(vs, axis=0)
        t_ref[pl.ds(start, G), :] = v_all
        both = jnp.concatenate([u_all, v_all], axis=1)
        high = both.astype(BF16).astype(F32)
        low = both - high
        lhs = jnp.concatenate([high[:, :TILE], high[:, :TILE], low[:, :TILE]], axis=0)
        rhs = jnp.concatenate([high, low, high], axis=0)
        d_ref[...] -= dot(lhs.astype(BF16), rhs.astype(BF16), ((0,), (0,)))
        for k, stages in enumerate(hooks):
            if stages:
                @pl.when(g == k)
                def _():
                    for stage in stages:
                        stage()
        return carry

    lax.fori_loop(0, TILE // G, step, 0)


def ace_kernel(bands, groups, orb, kern, blk, ace, exch, full, extra, w, wx, a, rest, x16, xlow, mba,
               d_ref, t_ref, proj, proj2, bfull, acc, applied, loc, m_s, m_r, n_s, n_r, c_s, c_r,
               d_s, d_r, b_s, b_r, p_s, p_r, t_s, t_r, e_s, e_r, *scratch):
    at = Place(bands, groups)
    me, team = at.me, at.team
    own, bown = ace.shape[0], exch.shape[0]
    cols = w.shape[1]
    n, nblk = own * bands, bown * bands
    n2 = n // 2
    scale = 1.0 / (ace.shape[1] * groups)
    inner = Reduce(at, scratch[:SCRATCH], True)
    cross = Reduce(at, scratch[SCRATCH:2 * SCRATCH], False)
    couple = Reduce(at, scratch[2 * SCRATCH:], False)
    greet(at.everyone())

    def chunk(index):
        return pl.ds(pl.multiple_of(index * cols, TILE), cols)

    def twin(index):
        return chunk(lax.rem(index + team, bands))

    mine = full.at[span(me, own)]
    also = extra.at[span(me, own)]
    bmine = bfull.at[span(me, bown)]

    def kept():
        return [pltpu.make_async_copy(orb.at[:, chunk(me)], mine, loc.at[0]),
                pltpu.make_async_copy(orb.at[:, twin(me)], also, loc.at[1])]

    def to_mates():
        copies = []
        for j in range(1, team):
            p = at.half * team + at.mate(j)
            copies.append(remote(orb.at[:, chunk(p)], mine, m_s.at[j], m_r.at[j], {"band": p}))
            copies.append(remote(orb.at[:, twin(p)], also, n_s.at[j], n_r.at[j], {"band": p}))
        return copies

    def to_rival(t, sender):
        p = at.rival(t)
        return remote(orb.at[:, chunk(p)], mine, c_s.at[t], c_r.at[sender], {"band": p})

    def twin_rival(t, sender, lo=0, size=own):
        p = at.rival(t)
        return remote(orb.at[pl.ds(lo, size), twin(p)], extra.at[span(me, size, lo, own)],
                      d_s.at[t], d_r.at[sender], {"band": p})

    slices = [(t, lo) for lo in range(0, own, SLICE) for t in range(team)]

    def upward(count):
        def go():
            @pl.when(at.half == 0)
            def _():
                for t, lo in batch:
                    twin_rival(t, at.rank, lo, SLICE).start()
        batch, slices[:] = slices[:count], slices[count:]
        return go

    def blocks():
        return [remote(blk.at[:, chunk(at.peer[d])], bmine, b_s.at[d], b_r.at[d], at.band(d))
                for d in at.far]

    def bkept():
        return pltpu.make_async_copy(blk.at[:, chunk(me)], bmine, loc.at[2])

    for copy in to_mates():
        copy.start()
    for t in range(team):
        to_rival(t, at.rank).start()
    for copy in kept():
        copy.start()
    bkept().start()

    def weigh(rows, columns):
        return (-(rows.astype(F32) * kern[:, columns])).astype(BF16)

    for copy in kept() + to_mates():
        copy.wait()
    band = span(at.half, n2)
    w[band, :] = weigh(full[band, :], chunk(me))
    wx[band, :] = weigh(extra[band, :], twin(me))
    row = 0
    for s in range(0, n2, TILE):
        e = s + TILE
        product = (dot(w[span(at.half, TILE, s, n2), :], full[span(at.half, e, 0, n2), :],
                       ((1,), (1,)))
                   + dot(wx[span(at.half, TILE, s, n2), :], extra[span(at.half, e, 0, n2), :],
                         ((1,), (1,))))
        for c in range(0, e, TILE):
            inner.put(row, product[:, c:c + TILE])
            row += TILE
    inner.pad(row)
    inner.s1()
    inner.s2()
    inner.s3()
    inner.s4()
    for t in range(team):
        to_rival(t, t).wait_recv()
    other = span(1 - at.half, n2)
    w[other, :] = weigh(full[other, :], chunk(me))
    row = 0
    for s in range(n2, n, TILE):
        product = dot(w[s:s + TILE, :], full[0:n2, :], ((1,), (1,)))
        for c in range(0, n2, TILE):
            cross.put(row, product[:, c:c + TILE])
            row += TILE
    cross.pad(row)
    cross.s1()
    inner.s5()
    for copy in blocks():
        copy.start()
    cross.s2()
    inner.s6()
    inner.s7()
    row = 0
    for base in (0, n2):
        for s in range(base, base + n2, TILE):
            for c in range(base, s + TILE, TILE):
                a[s:s + TILE, c:c + TILE] = inner.allg[row:row + TILE, :].astype(F32) * -scale
                row += TILE
        row = inner.rows
    rest[...] = identity(n)
    x16[...] = jnp.zeros_like(x16)
    xlow[...] = jnp.zeros_like(xlow)

    def couple_start():
        bkept().wait()
        for copy in blocks():
            copy.wait()
        half = nblk // 2
        for h in range(2):
            couple.put(h * n, dot(w[...], bfull[h * half:(h + 1) * half, :], ((1,), (1,))))
        couple.s1()

    cuts = sorted(set(range(0, n, TILE)) | set(range(0, n, own)) | {n})
    pieces = list(enumerate(zip(cuts[:-1], cuts[1:])))

    def piece(q, r0, r1, source, target, other):
        lo = r0 % own
        rows, sent, got = (proj2, t_s, t_r) if other else (proj, p_s, p_r)
        where = twin(source) if other else chunk(source)
        return remote(rows.at[r0:r1], ace.at[lo:lo + r1 - r0, where],
                      sent.at[q], got.at[q, source], {"band": target})

    def stay(q, r0, r1, other):
        lo = r0 % own
        rows, sent = (proj2, t_s) if other else (proj, p_s)
        where = twin(me) if other else chunk(me)
        return pltpu.make_async_copy(rows.at[r0:r1], ace.at[lo:lo + r1 - r0, where], sent.at[q])

    def deliver(lo, hi, other):
        for q, (r0, r1) in pieces:
            if lo <= r0 < hi:
                owner = r0 // own

                @pl.when((me != owner) & (at.half == owner // team))
                def _():
                    piece(q, r0, r1, me, owner, other).start()

                @pl.when(me == owner)
                def _():
                    stay(q, r0, r1, other).start()

    def project(lo, hi):
        proj2[lo:hi, :] = (dot(x16[lo:hi, 0:hi], wx[0:hi, :], ((1,), (0,)))
                           + dot(xlow[lo:hi, 0:hi], wx[0:hi, :], ((1,), (0,)))).astype(BF16)

    def spare():
        @pl.when(at.half == 0)
        def _():
            project(0, n2)

        for other in (0, 1):
            deliver(0, n2, other)

    def arrive():
        @pl.when(at.half == 1)
        def _():
            for t in range(team):
                twin_rival(t, t).wait_recv()
            wx[0:n2, :] = weigh(extra[0:n2, :], twin(me))

    tiles = n2 // TILE
    hooks = [[[] for _ in range(4)] for _ in range(2 * tiles)]

    def at_hook(k, g, *stages):
        hooks[k][g] += stages

    for g in range(4):
        at_hook(0, g, upward(1))
        at_hook(tiles - 2, g, upward(1))
        at_hook(tiles - 1, g, upward(1))
    at_hook(0, 1, cross.s3)
    at_hook(tiles - 2, 0, couple_start)
    at_hook(tiles - 2, 1, cross.s4)
    at_hook(tiles - 2, 3, couple.s2)
    at_hook(tiles - 1, 0, cross.s5)
    at_hook(tiles - 1, 1, couple.s3)
    at_hook(tiles - 1, 2, cross.s6)
    at_hook(tiles, 1, couple.s5, upward(len(slices)), spare)
    at_hook(tiles, 3, couple.s6)
    at_hook(tiles + 1, 0, couple.s7)

    def attach(lo, hi):
        half = nblk // 2
        for h in range(2):
            part = allg_dot(lo, hi, h) * scale
            update = dot(part.astype(BF16), proj[lo:hi, :], ((0,), (0,)))
            if lo == 0:
                acc[h * half:(h + 1) * half, :] = update
            else:
                acc[h * half:(h + 1) * half, :] += update

    def allg_dot(lo, hi, h):
        return dot(x16[lo:hi, 0:hi], couple.allg[h * n:h * n + hi, :], ((1,), (0,)))

    for k, s in enumerate(range(0, n, TILE)):
        e = s + TILE
        top = n2 if s < n2 else n
        d_ref[:, 0:TILE] = a[s:e, s:e]
        d_ref[:, TILE:] = identity(TILE)
        factor_tile(d_ref, t_ref, hooks[k])
        tile = t_ref[...]
        rows = product3(tile, rest[s:e, 0:e], ((1,), (0,)))
        high, low = split(rows)
        x16[s:e, 0:e] = high
        xlow[s:e, 0:e] = low
        proj[s:e, :] = (dot(high, w[0:e, :], ((1,), (0,)))
                        + dot(low, w[0:e, :], ((1,), (0,)))).astype(BF16)
        if s >= n2:
            deliver(s, e, 0)
        if e < top:
            panel = product3(a[e:top, s:e], tile, ((1,), (1,)))
            for c in range(e, top, TILE):
                a[c:top, c:c + TILE] -= product3(panel[c - e:], panel[c - e:c - s], ((1,), (1,)))
            rest[e:top, 0:e] -= product3(panel, rows, ((1,), (0,)))
        if e == n2:
            cross.s7()
            row = 0
            for r in range(0, n2, TILE):
                for c in range(0, n2, TILE):
                    mba[r:r + TILE, c:c + TILE] = cross.allg[row:row + TILE, :]
                    row += TILE
            both = (((1,), (1,)))
            below = (dot(mba[...], x16[0:n2, 0:n2], both) + dot(mba[...], xlow[0:n2, 0:n2], both)) * -scale
            bh, bl = split(below)
            for c in range(0, n2, TILE):
                d = c + TILE
                a[n2 + c:n, n2 + c:n2 + d] -= (
                    dot(bh[c:], bh[c:d], both) + (dot(bh[c:], bl[c:d], both) + dot(bl[c:], bh[c:d], both)))
            over = ((1,), (0,))
            xh = x16[0:n2, 0:n2]
            rest[n2:, 0:n2] = -(dot(bh, xh, over) + (dot(bh, xlow[0:n2, 0:n2], over) + dot(bl, xh, over)))
            couple.s4()
        if e == n - TILE:
            attach(0, e)
    attach(n - TILE, n)
    applied[...] = (-acc[...]).astype(BF16)
    outs = [remote(applied.at[span(at.peer[d], bown)], exch.at[:, chunk(me)],
                   e_s.at[d], e_r.at[d], at.band(d)) for d in at.far]
    outs.append(pltpu.make_async_copy(applied.at[span(me, bown)], exch.at[:, chunk(me)], loc.at[3]))
    for copy in outs:
        copy.start()
    arrive()

    @pl.when(at.half == 1)
    def _():
        project(n2, n)

    deliver(n2, n, 1)
    for t in range(team):
        to_rival(t, t).wait_send()

    @pl.when(at.half == 0)
    def _():
        for t in range(team):
            twin_rival(t, t).wait_send()

    for q, (r0, r1) in pieces:
        owner = r0 // own

        @pl.when((me != owner) & (at.half == owner // team))
        def _():
            for other in (0, 1):
                piece(q, r0, r1, me, owner, other).wait_send()

        @pl.when(me == owner)
        def _():
            for other in (0, 1):
                stay(q, r0, r1, other).wait()
                for j in range(1, team):
                    mate = at.half * team + at.mate(j)
                    piece(q, r0, r1, mate, mate, other).wait_recv()
    for copy in outs:
        copy.wait()


def shards(orbitals, kernel, block_vectors):
    groups, bands = lax.axis_size("ga"), lax.axis_size("band")
    own, width = orbitals.shape
    bown = block_vectors.shape[0]
    cols = width // bands
    n, nblk = own * bands, bown * bands
    n2, team = n // 2, bands // 2
    levels = max(groups.bit_length() - 3, 1)
    tiles = n2 // TILE

    def padded(rows, parts):
        unit = 4 * parts * 16
        return -(-rows // unit) * unit

    pieces = len(set(range(0, n, TILE)) | set(range(0, n, own)))
    vmem, hbm = pl.BlockSpec(memory_space=pltpu.VMEM), pl.BlockSpec(memory_space=pl.ANY)
    dma = pltpu.SemaphoreType.DMA
    many, some = dma((bands,)), dma((team,))
    return pl.pallas_call(
        functools.partial(ace_kernel, bands, groups),
        name="ace",
        out_shape=(
            jax.ShapeDtypeStruct((own, width), BF16),
            jax.ShapeDtypeStruct((bown, width), BF16),
        ),
        in_specs=[hbm, vmem, hbm],
        out_specs=(hbm, hbm),
        scratch_shapes=[
            pltpu.VMEM((n, cols), BF16),
            pltpu.VMEM((n, cols), BF16),
            pltpu.VMEM((n, cols), BF16),
            pltpu.VMEM((n, cols), BF16),
            pltpu.VMEM((n, n), F32),
            pltpu.VMEM((n, n), F32),
            pltpu.VMEM((n, n), BF16),
            pltpu.VMEM((n, n), BF16),
            pltpu.VMEM((n2, n2), BF16),
            pltpu.VMEM((TILE, 2 * TILE), F32),
            pltpu.VMEM((TILE, TILE), F32),
            pltpu.VMEM((n, cols), BF16),
            pltpu.VMEM((n, cols), BF16),
            pltpu.VMEM((nblk, cols), BF16),
            pltpu.VMEM((nblk, cols), F32),
            pltpu.VMEM((nblk, cols), BF16),
            dma((4,)), some, some, some, some, some, some, some, some,
            many, many, dma((pieces,)), dma((pieces, bands)), dma((pieces,)), dma((pieces, bands)),
            many, many,
        ]
        + reduce_scratch(padded(tiles * (tiles + 1) // 2 * TILE, team), team, bands, levels, 2)
        + reduce_scratch(padded(tiles * tiles * TILE, bands), bands, bands, levels, 1)
        + reduce_scratch(2 * n, bands, bands, levels, 1),
        compiler_params=pltpu.CompilerParams(
            collective_id=0, has_side_effects=True, vmem_limit_bytes=56 * 2**20),
    )(orbitals, kernel.reshape(1, width), block_vectors)


def solution(mesh):
    placed = (P(("img", "band"), "ga"), P("ga"), P(("img", "band"), "ga"))
    return jax.shard_map(
        shards,
        mesh=mesh,
        in_specs=placed,
        out_specs=(P(("img", "band"), "ga"), P(("img", "band"), "ga")),
        check_vma=False,
    )
```

```python
import functools

import jax
import jax.numpy as jnp
from jax import lax
from jax.experimental import pallas as pl
from jax.experimental.pallas import tpu as pltpu
from jax.sharding import PartitionSpec as P

MESH = pl.DeviceIdType.MESH
F32 = jnp.float32
BF16 = jnp.bfloat16
TILE = 128
LANES = 128


def remote(src, dst, send_sem, recv_sem, where):
    return pltpu.make_async_remote_copy(
        src_ref=src, dst_ref=dst, send_sem=send_sem, recv_sem=recv_sem,
        device_id=where, device_id_type=MESH,
    )


def greet(places):
    barrier = pltpu.get_barrier_semaphore()
    for place in places:
        pl.semaphore_signal(barrier, inc=1, device_id=place, device_id_type=MESH)
    pl.semaphore_wait(barrier, len(places))


def dot(a, b, dims):
    return lax.dot_general(a, b, (dims, ((), ())), preferred_element_type=F32)


class Place:
    def __init__(self, bands, groups):
        self.bands = bands
        self.me = lax.axis_index("band")
        self.team = bands // 2
        self.half = self.me // self.team
        self.rank = lax.rem(self.me, self.team)
        ga = lax.axis_index("ga")
        self.core = lax.rem(ga, 2)
        self.row = lax.rem(ga // 2, 2)
        self.partner = {"ga": ga + 1 - 2 * self.core}
        self.across = {"ga": ga + 2 - 4 * self.row}
        self.peer = [lax.rem(self.me + d, bands) for d in range(bands)]
        self.far = sorted(range(1, bands), key=lambda d: -min(d, bands - d))
        self.near = self.far[::-1]
        self.bits = []
        stride = 4
        while stride < groups:
            self.bits.append({"ga": ga + stride * (1 - 2 * lax.rem(ga // stride, 2))})
            stride *= 2

    def band(self, d):
        return {"band": self.peer[d]}

    def mate(self, j):
        return lax.rem(self.rank + j, self.team)

    def rival(self, t):
        return (1 - self.half) * (self.team + t) + self.half * (self.team - 1 - t)

    def everyone(self):
        return [self.band(d) for d in range(1, self.bands)] + [self.partner, self.across] + self.bits


def span(index, size, offset=0, stride=None):
    return pl.ds(pl.multiple_of(offset + index * (stride or size), 16), size)


def reduce_scratch(rows, parts, bands, levels, sides):
    h1, h2 = rows // 2, rows // 4
    h3 = h2 // parts
    dma = pltpu.SemaphoreType.DMA
    shapes = [
        ((rows, TILE), F32), ((rows, TILE), BF16), ((h1, TILE), BF16),
        ((h1, TILE), F32), ((h1, TILE), BF16), ((h2, TILE), BF16),
        ((h2, TILE), F32), ((h2, TILE), BF16), ((parts, h3, TILE), BF16),
        ((levels, h3, TILE), BF16), ((levels, h3, TILE), BF16), ((sides * rows, TILE), BF16),
    ]
    return [pltpu.VMEM(*shape) for shape in shapes] + [
        dma((4,)), dma((parts,)), dma((parts,)), dma((levels,)), dma((levels,)),
        dma((bands,)), dma((bands,)), dma((bands,)), dma((bands,)),
        dma((2 * bands,)), dma((2 * bands,)),
    ]


SCRATCH = 23


class Reduce:
    def __init__(self, at, scratch, by_team):
        self.at = at
        (self.p32, self.p16, self.rx1, self.a32, self.a16, self.rx2, self.b32, self.b16, self.rx3,
         self.out_x, self.rx_x, self.allg, self.one, self.z_s, self.z_r, self.x_s, self.x_r,
         self.g_s, self.g_r, self.y_s, self.y_r, self.f_s, self.f_r) = scratch
        self.rows = self.p32.shape[0]
        self.h1, self.h2, self.h3 = self.rx1.shape[0], self.rx2.shape[0], self.rx3.shape[1]
        self.by_team = by_team
        if by_team:
            self.mine = at.rank
            self.parts = [(j, at.mate(j), {"band": at.half * at.team + at.mate(j)})
                          for j in range(1, at.team)]
        else:
            self.mine = at.me
            self.parts = [(d, at.peer[d], at.band(d)) for d in at.far]

    def put(self, row, value):
        size = value.shape[0]
        self.p32[row:row + size, :] = value
        self.p16[row:row + size, :] = value.astype(BF16)

    def pad(self, row):
        size = self.rows - row
        if size:
            self.put(row, jnp.zeros((size, TILE), F32))

    def to_partner(self):
        at = self.at
        return remote(self.p16.at[span(1 - at.core, self.h1)], self.rx1,
                      self.one.at[0], self.one.at[1], at.partner)

    def to_across(self):
        at = self.at
        return remote(self.a16.at[span(1 - at.row, self.h2)], self.rx2,
                      self.one.at[2], self.one.at[3], at.across)

    def to_parts(self):
        return [remote(self.b16.at[span(index, self.h3)], self.rx3.at[slot],
                       self.z_s.at[slot], self.z_r.at[slot], where)
                for slot, index, where in self.parts]

    def piece(self, d, row):
        at = self.at
        source = lax.rem(at.me + at.bands - d, at.bands)
        offset = at.core * self.h1 + row * self.h2
        if self.by_team:
            offset = offset + (source // at.team) * self.rows
            source = lax.rem(source, at.team)
        return span(source, self.h3, offset)

    def gather(self, d):
        own = self.allg.at[self.piece(0, self.at.row)]
        return remote(own, own, self.g_s.at[d], self.g_r.at[d], self.at.band(d))

    def side(self, d):
        there = self.allg.at[self.piece(d, self.at.row)]
        return remote(there, there, self.y_s.at[d], self.y_r.at[d], self.at.across)

    def last(self, d, other):
        row = 1 - self.at.row if other else self.at.row
        there = self.allg.at[self.piece(d, row)]
        e = d + self.at.bands * other
        return remote(there, there, self.f_s.at[e], self.f_r.at[e], self.at.partner)

    def s1(self):
        self.to_partner().start()

    def s2(self):
        self.to_partner().wait()
        self.a32[...] = self.p32[span(self.at.core, self.h1), :] + self.rx1[...].astype(F32)
        self.a16[...] = self.a32[...].astype(BF16)
        self.to_across().start()

    def s3(self):
        self.to_across().wait()
        self.b32[...] = self.a32[span(self.at.row, self.h2), :] + self.rx2[...].astype(F32)
        self.b16[...] = self.b32[...].astype(BF16)
        for copy in self.to_parts():
            copy.start()

    def s4(self):
        at = self.at
        for copy in self.to_parts():
            copy.wait()
        total = self.b32[span(self.mine, self.h3), :]
        for slot, _, _ in self.parts:
            total = total + self.rx3[slot].astype(F32)
        for i, place in enumerate(at.bits):
            self.out_x[i] = total.astype(BF16)
            copy = remote(self.out_x.at[i], self.rx_x.at[i], self.x_s.at[i], self.x_r.at[i], place)
            copy.start()
            copy.wait()
            total = self.out_x[i].astype(F32) + self.rx_x[i].astype(F32)
        self.allg[self.piece(0, at.row), :] = total.astype(BF16)
        for d in at.far:
            self.gather(d).start()
        self.side(0).start()
        self.last(0, 0).start()

    def s5(self):
        for d in self.at.near:
            self.gather(d).wait()
            self.side(d).start()
            self.last(d, 0).start()

    def s6(self):
        for d in [0] + self.at.near:
            self.side(d).wait()
            self.last(d, 1).start()

    def s7(self):
        for d in [0] + self.at.near:
            self.last(d, 0).wait()
            self.last(d, 1).wait()


def split(a):
    high = a.astype(BF16)
    return high, (a - high.astype(F32)).astype(BF16)


def product3(a, b, dims):
    (ah, al), (bh, bl) = split(a), split(b)
    return dot(ah, bh, dims) + (dot(ah, bl, dims) + dot(al, bh, dims))


def identity(rows):
    shape = (rows, rows)
    return (lax.broadcasted_iota(jnp.int32, shape, 0)
            == lax.broadcasted_iota(jnp.int32, shape, 1)).astype(F32)


def factor_tile(d_ref, t_ref, hooks):
    G, SUB, BLK = 32, 8, 16
    H, K = G // SUB, BLK // SUB
    sub = lax.broadcasted_iota(jnp.int32, (SUB, TILE), 0)

    def spread(block, i):
        return jnp.broadcast_to(block[i:i + 1, :], (SUB, TILE))

    def lane(block, c):
        where = jnp.full((SUB, TILE), c, jnp.int32)
        return jnp.take_along_axis(block, where, axis=1, mode="promise_in_bounds")

    def step(g, carry):
        start = g * G if isinstance(g, int) else pl.multiple_of(g * G, G)
        lefts = [d_ref[pl.ds(start + h * SUB, SUB), 0:TILE] for h in range(H)]
        rights = [d_ref[pl.ds(start + h * SUB, SUB), TILE:2 * TILE] for h in range(H)]
        us, vs = [None] * H, [None] * H
        for b in range(G // BLK):
            h0 = b * K
            cols = [{h: lane(lefts[h], start + (b * BLK + c)) for h in range(h0 + c // SUB, H)}
                    for c in range(BLK)]
            pivot = spread(cols[0][h0], 0)
            for j in range(BLK):
                k, i = h0 + j // SUB, j % SUB
                r = lax.rsqrt(pivot)
                low = {c: spread(cols[j][h0 + c // SUB], c % SUB) for c in range(j + 1, BLK)}
                if j + 1 < BLK:
                    low[j + 1] = low[j + 1] * r
                    pivot = spread(cols[j + 1][h0 + (j + 1) // SUB], (j + 1) % SUB) - low[j + 1] * low[j + 1]
                for h in range(k, H):
                    cols[j][h] = cols[j][h] * r
                u, v = spread(lefts[k], i) * r, spread(rights[k], i) * r
                us[k] = u if i == 0 else jnp.where(sub == i, u, us[k])
                vs[k] = v if i == 0 else jnp.where(sub == i, v, vs[k])
                for c in range(j + 1, BLK):
                    scaled = low[c] if c == j + 1 else low[c] * r
                    for h in range(h0 + c // SUB, H):
                        cols[c][h] = cols[c][h] - cols[j][h] * scaled
                for h in range(k if i < SUB - 1 else k + 1, H):
                    lefts[h] = lefts[h] - cols[j][h] * u
                    rights[h] = rights[h] - cols[j][h] * v
        u_all = jnp.concatenate(us, axis=0)
        v_all = jnp.concatenate(vs, axis=0)
        t_ref[pl.ds(start, G), :] = v_all
        if isinstance(g, int):
            for stage in hooks[g]:
                stage()
            return carry
        both = jnp.concatenate([u_all, v_all], axis=1)
        high = both.astype(BF16).astype(F32)
        low = both - high
        lhs = jnp.concatenate([high[:, :TILE], high[:, :TILE], low[:, :TILE]], axis=0)
        rhs = jnp.concatenate([high, low, high], axis=0)
        d_ref[...] -= dot(lhs.astype(BF16), rhs.astype(BF16), ((0,), (0,)))
        for k, stages in enumerate(hooks[:-1]):
            if stages:
                @pl.when(g == k)
                def _():
                    for stage in stages:
                        stage()
        return carry

    lax.fori_loop(0, TILE // G - 1, step, 0)
    step(TILE // G - 1, 0)


def ace_kernel(bands, groups, orb, kern, blk, ace, exch, full, extra, w, wx, a, rest, x16, xlow, mba,
               d_ref, t_ref, proj, proj2, bfull, acc, applied, applied2, back, loc, m_s, m_r, n_s, n_r, c_s, c_r,
               d_s, d_r, b_s, b_r, p_s, p_r, t_s, t_r, e_s, e_r, f_s, f_r, *scratch):
    at = Place(bands, groups)
    me, team = at.me, at.team
    own, bown = ace.shape[0], exch.shape[0]
    cols = w.shape[1]
    n, nblk = own * bands, bown * bands
    n2 = n // 2
    scale = 1.0 / (ace.shape[1] * groups)
    inner = Reduce(at, scratch[:SCRATCH], True)
    cross = Reduce(at, scratch[SCRATCH:2 * SCRATCH], False)
    couple = Reduce(at, scratch[2 * SCRATCH:], False)
    greet(at.everyone())

    def chunk(index):
        return pl.ds(pl.multiple_of(index * cols, TILE), cols)

    def twin(index):
        return chunk(lax.rem(index + team, bands))

    mine = full.at[span(me, own)]
    also = extra.at[span(me, own)]
    bmine = bfull.at[span(me, bown)]

    def kept():
        return [pltpu.make_async_copy(orb.at[:, chunk(me)], mine, loc.at[0]),
                pltpu.make_async_copy(orb.at[:, twin(me)], also, loc.at[1])]

    def to_mates():
        copies = []
        for j in range(1, team):
            p = at.half * team + at.mate(j)
            copies.append(remote(orb.at[:, chunk(p)], mine, m_s.at[j], m_r.at[j], {"band": p}))
            copies.append(remote(orb.at[:, twin(p)], also, n_s.at[j], n_r.at[j], {"band": p}))
        return copies

    def to_rival(t, sender):
        p = at.rival(t)
        return remote(orb.at[:, chunk(p)], mine, c_s.at[t], c_r.at[sender], {"band": p})

    parts = [(0, cols // 2 // LANES * LANES), (cols // 2 // LANES * LANES, cols)]
    parts = [part for part in parts if part[0] < part[1]]

    def twin_rival(t, sender, lo, hi):
        p = at.rival(t)
        first = pl.multiple_of(lax.rem(p + team, bands) * cols + lo, TILE)
        k = 0 if hi <= parts[0][1] else 1
        return remote(orb.at[:, pl.ds(first, hi - lo)], extra.at[span(me, own), lo:hi],
                      d_s.at[t, k], d_r.at[sender, k], {"band": p})

    slices = [(t, lo) for lo in range(0, cols, LANES) for t in range(team)]
    left = {True: list(slices), False: list(slices)}
    near = at.rank >= team // 2

    def upward(count, first=True):
        batch, left[first][:] = left[first][:count], left[first][count:]

        def go():
            @pl.when((at.half == 0) & (near if first else ~near))
            def _():
                for t, lo in batch:
                    twin_rival(t, at.rank, lo, lo + LANES).start()
        return go

    def block(slot, p, sender):
        return remote(blk.at[:, chunk(p)], bmine, b_s.at[slot], b_r.at[sender], {"band": p})

    def block_rival(t):
        return lambda: block(t, at.rival(t), me).start()

    def block_mates():
        for j in range(1, team):
            block(team + j, at.half * team + at.mate(j), me).start()

    def bkept():
        return pltpu.make_async_copy(blk.at[:, chunk(me)], bmine, loc.at[2])

    for copy in to_mates():
        copy.start()
    for t in range(team):
        to_rival(t, at.rank).start()
    for copy in kept():
        copy.start()
    bkept().start()

    def weigh(rows, columns):
        return (-(rows.astype(F32) * kern[:, columns])).astype(BF16)

    for copy in kept() + to_mates():
        copy.wait()
    band = span(at.half, n2)
    w[band, :] = weigh(full[band, :], chunk(me))
    wx[band, :] = weigh(extra[band, :], twin(me))
    row = 0
    for s in range(0, n2, TILE):
        e = s + TILE
        product = (dot(w[span(at.half, TILE, s, n2), :], full[span(at.half, e, 0, n2), :],
                       ((1,), (1,)))
                   + dot(wx[span(at.half, TILE, s, n2), :], extra[span(at.half, e, 0, n2), :],
                         ((1,), (1,))))
        for c in range(0, e, TILE):
            inner.put(row, product[:, c:c + TILE])
            row += TILE
    inner.pad(row)
    inner.s1()
    inner.s2()
    inner.s3()
    inner.s4()
    for t in range(team):
        to_rival(t, t).wait_recv()
    other = span(1 - at.half, n2)
    w[other, :] = weigh(full[other, :], chunk(me))
    row = 0
    for s in range(n2, n, TILE):
        product = dot(w[s:s + TILE, :], full[0:n2, :], ((1,), (1,)))
        for c in range(0, n2, TILE):
            cross.put(row, product[:, c:c + TILE])
            row += TILE
    cross.pad(row)
    cross.s1()
    for t in range(team - 1):
        block_rival(t)()
    cross.s2()
    inner.s5()
    cross.s3()
    block_rival(team - 1)()
    block_mates()
    inner.s6()
    inner.s7()
    row = 0
    for base in (0, n2):
        for s in range(base, base + n2, TILE):
            for c in range(base, s + TILE, TILE):
                a[s:s + TILE, c:c + TILE] = inner.allg[row:row + TILE, :].astype(F32) * -scale
                row += TILE
        row = inner.rows
    rest[...] = identity(n)
    x16[...] = jnp.zeros_like(x16)
    xlow[...] = jnp.zeros_like(xlow)

    def couple_start():
        bkept().wait()
        for d in range(1, bands):
            block(d, at.peer[d], at.peer[d]).wait_recv()
        half = nblk // 2
        for h in range(2):
            couple.put(h * n, dot(w[...], bfull[h * half:(h + 1) * half, :], ((1,), (1,))))
        couple.s1()

    cuts = sorted(set(range(0, n, TILE)) | set(range(0, n, own)) | {n})
    pieces = list(enumerate(zip(cuts[:-1], cuts[1:])))

    def piece(q, r0, r1, source, target, other):
        lo = r0 % own
        if other:
            return strip(q, r0, r1, source, target, 0, 0, cols)
        return remote(proj.at[r0:r1], ace.at[lo:lo + r1 - r0, chunk(source)],
                      p_s.at[q], p_r.at[q, source], {"band": target})

    def stay(q, r0, r1, other):
        lo = r0 % own
        if other:
            return strip_stay(q, r0, r1, 0, 0, cols)
        return pltpu.make_async_copy(
            proj.at[r0:r1], ace.at[lo:lo + r1 - r0, chunk(me)], p_s.at[q])

    def some(source, c0, c1):
        first = lax.rem(source + team, bands) * cols + c0
        return pl.ds(pl.multiple_of(first, TILE), c1 - c0)

    def strip(q, r0, r1, source, target, k, c0, c1):
        lo = r0 % own
        return remote(proj2.at[r0:r1, c0:c1], ace.at[lo:lo + r1 - r0, some(source, c0, c1)],
                      t_s.at[q, k], t_r.at[q, source, k], {"band": target})

    def strip_stay(q, r0, r1, k, c0, c1):
        lo = r0 % own
        return pltpu.make_async_copy(
            proj2.at[r0:r1, c0:c1], ace.at[lo:lo + r1 - r0, some(me, c0, c1)], t_s.at[q, k])

    def deliver(lo, hi, other):
        for q, (r0, r1) in pieces:
            if lo <= r0 < hi:
                owner = r0 // own

                @pl.when((me != owner) & (at.half == owner // team))
                def _():
                    piece(q, r0, r1, me, owner, other).start()

                @pl.when(me == owner)
                def _():
                    stay(q, r0, r1, other).start()

    def project(lo, hi, c0, c1):
        proj2[lo:hi, c0:c1] = (dot(x16[lo:hi, 0:hi], wx[0:hi, c0:c1], ((1,), (0,)))
                               + dot(xlow[lo:hi, 0:hi], wx[0:hi, c0:c1], ((1,), (0,)))).astype(BF16)

    def spare():
        @pl.when(at.half == 0)
        def _():
            project(0, n2, 0, cols)

        deliver(0, n2, 1)

    tiles = n2 // TILE
    hooks = [[[] for _ in range(4)] for _ in range(2 * tiles)]

    def at_hook(k, g, *stages):
        hooks[k][g] += stages

    at_hook(0, 2, cross.s4)
    at_hook(tiles - 2, 0, couple_start)
    at_hook(tiles - 2, 2, couple.s2)
    at_hook(tiles - 2, 3, cross.s5, upward(1), upward(1, False))
    at_hook(tiles - 1, 0, upward(1), upward(1, False))
    at_hook(tiles - 1, 1, upward(1))
    at_hook(tiles - 1, 3, couple.s3, cross.s6)
    at_hook(tiles, 0, upward(len(slices)))
    at_hook(tiles + 1, 1, couple.s5, upward(len(slices), False), spare)
    at_hook(tiles + 2, 1, couple.s6)
    at_hook(tiles + 2, 3, couple.s7)

    def attach(lo, hi):
        half = nblk // 2
        for h in range(2):
            part = allg_dot(lo, hi, h) * scale
            update = dot(part.astype(BF16), proj[lo:hi, :], ((0,), (0,)))
            if lo == 0:
                acc[h * half:(h + 1) * half, :] = update
            else:
                acc[h * half:(h + 1) * half, :] += update

    def allg_dot(lo, hi, h):
        return dot(x16[lo:hi, 0:hi], couple.allg[h * n:h * n + hi, :], ((1,), (0,)))

    for k, s in enumerate(range(0, n, TILE)):
        e = s + TILE
        top = n2 if s < n2 else n
        d_ref[:, 0:TILE] = a[s:e, s:e]
        d_ref[:, TILE:] = identity(TILE)
        factor_tile(d_ref, t_ref, hooks[k])
        tile = t_ref[...]
        rows = product3(tile, rest[s:e, 0:e], ((1,), (0,)))
        high, low = split(rows)
        x16[s:e, 0:e] = high
        xlow[s:e, 0:e] = low
        proj[s:e, :] = (dot(high, w[0:e, :], ((1,), (0,)))
                        + dot(low, w[0:e, :], ((1,), (0,)))).astype(BF16)
        if s >= n2:
            deliver(s, e, 0)
        if e < top:
            panel = product3(a[e:top, s:e], tile, ((1,), (1,)))
            for c in range(e, top, TILE):
                a[c:top, c:c + TILE] -= product3(panel[c - e:], panel[c - e:c - s], ((1,), (1,)))
            rest[e:top, 0:e] -= product3(panel, rows, ((1,), (0,)))
        if e == n2:
            cross.s7()
            row = 0
            for r in range(0, n2, TILE):
                for c in range(0, n2, TILE):
                    mba[r:r + TILE, c:c + TILE] = cross.allg[row:row + TILE, :]
                    row += TILE
            both = (((1,), (1,)))
            below = (dot(mba[...], x16[0:n2, 0:n2], both) + dot(mba[...], xlow[0:n2, 0:n2], both)) * -scale
            bh, bl = split(below)
            for c in range(0, n2, TILE):
                d = c + TILE
                a[n2 + c:n, n2 + c:n2 + d] -= (
                    dot(bh[c:], bh[c:d], both) + (dot(bh[c:], bl[c:d], both) + dot(bl[c:], bh[c:d], both)))
            over = ((1,), (0,))
            xh = x16[0:n2, 0:n2]
            couple.s4()
            deliver(0, n2, 0)
            rest[n2:, 0:n2] = -(dot(bh, xh, over) + (dot(bh, xlow[0:n2, 0:n2], over) + dot(bl, xh, over)))
    attach(0, n)
    applied[...] = (-acc[...]).astype(BF16)

    def out(slot, p, sender):
        return remote(applied.at[span(p, bown)], exch.at[:, chunk(sender)],
                      e_s.at[slot], e_r.at[sender], {"band": p})

    def out2(slot, p, sender):
        return remote(applied2.at[span(lax.rem(p, team), bown)], exch.at[:, twin(sender)],
                      f_s.at[slot], f_r.at[sender], {"band": p})

    def held():
        return pltpu.make_async_copy(applied.at[span(me, bown)], exch.at[:, chunk(me)], loc.at[3])

    def held2():
        return pltpu.make_async_copy(applied2.at[span(at.rank, bown)], exch.at[:, twin(me)], loc.at[4])

    mates = [at.half * team + at.mate(j) for j in range(1, team)]

    @pl.when(at.half == 1)
    def _():
        for t in range(team):
            out(t, at.rival(t), me).start()

    for j, p in enumerate(mates):
        out(team + j, p, me).start()
    held().start()

    @pl.when(at.half == 1)
    def _():
        turned = ((0,), (0,))
        part = dot(x16[...], couple.allg[n:2 * n, :], ((1,), (0,))) * -scale
        ph, pq = split(part)
        back[...] = (dot(ph, x16[...], turned)
                     + (dot(ph, xlow[...], turned) + dot(pq, x16[...], turned)))

    @pl.when(at.half == 1)
    def _():
        bh, bl = split(back[...])
        forth = ((1,), (0,))
        for k, (c0, c1) in enumerate(parts):
            for t in range(team):
                twin_rival(t, t, c0, c1).wait_recv()
            wx[0:n2, c0:c1] = (-(extra[0:n2, c0:c1].astype(F32) * kern[:, some(me, c0, c1)])).astype(BF16)
            project(n2, n, c0, c1)
            for q, (r0, r1) in pieces:
                if r0 >= n2:
                    owner = r0 // own

                    @pl.when(me != owner)
                    def _():
                        strip(q, r0, r1, me, owner, k, c0, c1).start()

                    @pl.when(me == owner)
                    def _():
                        strip_stay(q, r0, r1, k, c0, c1).start()

            applied2[:, c0:c1] = (dot(bh, wx[:, c0:c1], forth) + dot(bl, wx[:, c0:c1], forth)).astype(BF16)
        for j, p in enumerate(mates):
            out2(j, p, me).start()
        held2().start()

    for t in range(team):
        to_rival(t, t).wait_send()
        block(t, me, me).wait_send()
    for j in range(1, team):
        block(team + j, me, me).wait_send()

    @pl.when(at.half == 0)
    def _():
        for t in range(team):
            for c0, c1 in parts:
                twin_rival(t, t, c0, c1).wait_send()

    for q, (r0, r1) in pieces:
        owner = r0 // own
        cells = list(enumerate(parts)) if r0 >= n2 else [(0, (0, cols))]

        @pl.when((me != owner) & (at.half == owner // team))
        def _():
            piece(q, r0, r1, me, owner, 0).wait_send()
            for k, (c0, c1) in cells:
                strip(q, r0, r1, me, owner, k, c0, c1).wait_send()

        @pl.when(me == owner)
        def _():
            stay(q, r0, r1, 0).wait()
            for k, (c0, c1) in cells:
                strip_stay(q, r0, r1, k, c0, c1).wait()
            for mate in mates:
                piece(q, r0, r1, mate, mate, 0).wait_recv()
                for k, (c0, c1) in cells:
                    strip(q, r0, r1, mate, mate, k, c0, c1).wait_recv()

    for j, p in enumerate(mates):
        out(team + j, p, p).wait()
    held().wait()

    @pl.when(at.half == 1)
    def _():
        for t in range(team):
            out(t, at.rival(t), me).wait_send()
        for j, p in enumerate(mates):
            out2(j, p, p).wait()
        held2().wait()

    @pl.when(at.half == 0)
    def _():
        for t in range(team):
            out(t, me, at.rival(t)).wait_recv()


def shards(orbitals, kernel, block_vectors):
    groups, bands = lax.axis_size("ga"), lax.axis_size("band")
    own, width = orbitals.shape
    bown = block_vectors.shape[0]
    cols = width // bands
    n, nblk = own * bands, bown * bands
    n2, team = n // 2, bands // 2
    levels = max(groups.bit_length() - 3, 1)
    tiles = n2 // TILE

    def padded(rows, parts):
        unit = 4 * parts * 16
        return -(-rows // unit) * unit

    pieces = len(set(range(0, n, TILE)) | set(range(0, n, own)))
    vmem, hbm = pl.BlockSpec(memory_space=pltpu.VMEM), pl.BlockSpec(memory_space=pl.ANY)
    dma = pltpu.SemaphoreType.DMA
    many, some = dma((bands,)), dma((team,))
    return pl.pallas_call(
        functools.partial(ace_kernel, bands, groups),
        name="ace",
        out_shape=(
            jax.ShapeDtypeStruct((own, width), BF16),
            jax.ShapeDtypeStruct((bown, width), BF16),
        ),
        in_specs=[hbm, vmem, hbm],
        out_specs=(hbm, hbm),
        scratch_shapes=[
            pltpu.VMEM((n, cols), BF16),
            pltpu.VMEM((n, cols), BF16),
            pltpu.VMEM((n, cols), BF16),
            pltpu.VMEM((n, cols), BF16),
            pltpu.VMEM((n, n), F32),
            pltpu.VMEM((n, n), F32),
            pltpu.VMEM((n, n), BF16),
            pltpu.VMEM((n, n), BF16),
            pltpu.VMEM((n2, n2), BF16),
            pltpu.VMEM((TILE, 2 * TILE), F32),
            pltpu.VMEM((TILE, TILE), F32),
            pltpu.VMEM((n, cols), BF16),
            pltpu.VMEM((n, cols), BF16),
            pltpu.VMEM((nblk, cols), BF16),
            pltpu.VMEM((nblk, cols), F32),
            pltpu.VMEM((nblk, cols), BF16),
            pltpu.VMEM((nblk // 2, cols), BF16),
            pltpu.VMEM((nblk // 2, n), F32),
            dma((5,)), some, some, some, some, some, some, dma((team, 2)), dma((team, 2)),
            many, many, dma((pieces,)), dma((pieces, bands)), dma((pieces, 2)), dma((pieces, bands, 2)),
            many, many, many, many,
        ]
        + reduce_scratch(padded(tiles * (tiles + 1) // 2 * TILE, team), team, bands, levels, 2)
        + reduce_scratch(padded(tiles * tiles * TILE, bands), bands, bands, levels, 1)
        + reduce_scratch(2 * n, bands, bands, levels, 1),
        compiler_params=pltpu.CompilerParams(
            collective_id=0, has_side_effects=True, vmem_limit_bytes=56 * 2**20),
    )(orbitals, kernel.reshape(1, width), block_vectors)


def solution(mesh):
    placed = (P(("img", "band"), "ga"), P("ga"), P(("img", "band"), "ga"))
    return jax.shard_map(
        shards,
        mesh=mesh,
        in_specs=placed,
        out_specs=(P(("img", "band"), "ga"), P(("img", "band"), "ga")),
        check_vma=False,
    )
```

```python
import functools

import jax
import jax.numpy as jnp
from jax import lax
from jax.experimental import pallas as pl
from jax.experimental.pallas import tpu as pltpu
from jax.sharding import PartitionSpec as P

MESH = pl.DeviceIdType.MESH
F32 = jnp.float32
BF16 = jnp.bfloat16
TILE = 128
LANES = 128


def remote(src, dst, send_sem, recv_sem, where):
    return pltpu.make_async_remote_copy(
        src_ref=src, dst_ref=dst, send_sem=send_sem, recv_sem=recv_sem,
        device_id=where, device_id_type=MESH,
    )


def greet(places):
    barrier = pltpu.get_barrier_semaphore()
    for place in places:
        pl.semaphore_signal(barrier, inc=1, device_id=place, device_id_type=MESH)
    pl.semaphore_wait(barrier, len(places))


def dot(a, b, dims):
    return lax.dot_general(a, b, (dims, ((), ())), preferred_element_type=F32)


class Place:
    def __init__(self, bands, groups):
        self.bands = bands
        self.me = lax.axis_index("band")
        self.team = bands // 2
        self.half = self.me // self.team
        self.rank = lax.rem(self.me, self.team)
        ga = lax.axis_index("ga")
        self.core = lax.rem(ga, 2)
        self.row = lax.rem(ga // 2, 2)
        self.partner = {"ga": ga + 1 - 2 * self.core}
        self.across = {"ga": ga + 2 - 4 * self.row}
        self.peer = [lax.rem(self.me + d, bands) for d in range(bands)]
        self.far = sorted(range(1, bands), key=lambda d: -min(d, bands - d))
        self.near = self.far[::-1]
        self.bits = []
        stride = 4
        while stride < groups:
            self.bits.append({"ga": ga + stride * (1 - 2 * lax.rem(ga // stride, 2))})
            stride *= 2

    def band(self, d):
        return {"band": self.peer[d]}

    def mate(self, j):
        return lax.rem(self.rank + j, self.team)

    def rival(self, t):
        return (1 - self.half) * (self.team + t) + self.half * (self.team - 1 - t)

    def everyone(self):
        return [self.band(d) for d in range(1, self.bands)] + [self.partner, self.across] + self.bits


def span(index, size, offset=0, stride=None):
    return pl.ds(pl.multiple_of(offset + index * (stride or size), 16), size)


def reduce_scratch(rows, parts, bands, levels, sides):
    h1, h2 = rows // 2, rows // 4
    h3 = h2 // parts
    dma = pltpu.SemaphoreType.DMA
    shapes = [
        ((rows, TILE), F32), ((rows, TILE), BF16), ((h1, TILE), BF16),
        ((h1, TILE), F32), ((h1, TILE), BF16), ((h2, TILE), BF16),
        ((h2, TILE), F32), ((h2, TILE), BF16), ((parts, h3, TILE), BF16),
        ((levels, h3, TILE), BF16), ((levels, h3, TILE), BF16), ((sides * rows, TILE), BF16),
    ]
    return [pltpu.VMEM(*shape) for shape in shapes] + [
        dma((4,)), dma((1,)), dma((1,)), dma((levels,)), dma((levels,)),
        dma((bands,)), dma((bands,)), dma((bands,)), dma((bands,)),
        dma((1,)), dma((1,)),
    ]


SCRATCH = 23


class Reduce:
    def __init__(self, at, scratch, by_team):
        self.at = at
        (self.p32, self.p16, self.rx1, self.a32, self.a16, self.rx2, self.b32, self.b16, self.rx3,
         self.out_x, self.rx_x, self.allg, self.one, self.z_s, self.z_r, self.x_s, self.x_r,
         self.g_s, self.g_r, self.y_s, self.y_r, self.f_s, self.f_r) = scratch
        self.rows = self.p32.shape[0]
        self.h1, self.h2, self.h3 = self.rx1.shape[0], self.rx2.shape[0], self.rx3.shape[1]
        self.by_team = by_team
        if by_team:
            self.mine = at.rank
            self.parts = [(j, at.mate(j), {"band": at.half * at.team + at.mate(j)})
                          for j in range(1, at.team)]
        else:
            self.mine = at.me
            self.parts = [(d, at.peer[d], at.band(d)) for d in at.far]

    def put(self, row, value):
        size = value.shape[0]
        self.p32[row:row + size, :] = value
        self.p16[row:row + size, :] = value.astype(BF16)

    def pad(self, row):
        size = self.rows - row
        if size:
            self.put(row, jnp.zeros((size, TILE), F32))

    def to_partner(self):
        at = self.at
        return remote(self.p16.at[span(1 - at.core, self.h1)], self.rx1,
                      self.one.at[0], self.one.at[1], at.partner)

    def to_across(self):
        at = self.at
        return remote(self.a16.at[span(1 - at.row, self.h2)], self.rx2,
                      self.one.at[2], self.one.at[3], at.across)

    def to_parts(self):
        return [remote(self.b16.at[span(index, self.h3)], self.rx3.at[slot],
                       self.z_s.at[0], self.z_r.at[0], where)
                for slot, index, where in self.parts]

    def piece(self, d, row):
        at = self.at
        source = lax.rem(at.me + at.bands - d, at.bands)
        offset = at.core * self.h1 + row * self.h2
        if self.by_team:
            offset = offset + (source // at.team) * self.rows
            source = lax.rem(source, at.team)
        return span(source, self.h3, offset)

    def gather(self, d):
        own = self.allg.at[self.piece(0, self.at.row)]
        return remote(own, own, self.g_s.at[d], self.g_r.at[d], self.at.band(d))

    def side(self, d):
        there = self.allg.at[self.piece(d, self.at.row)]
        return remote(there, there, self.y_s.at[d], self.y_r.at[d], self.at.across)

    def last(self, d, other):
        row = 1 - self.at.row if other else self.at.row
        there = self.allg.at[self.piece(d, row)]
        return remote(there, there, self.f_s.at[0], self.f_r.at[0], self.at.partner)

    def s1(self):
        self.to_partner().start()

    def s2(self):
        self.to_partner().wait()
        self.a32[...] = self.p32[span(self.at.core, self.h1), :] + self.rx1[...].astype(F32)
        self.a16[...] = self.a32[...].astype(BF16)
        self.to_across().start()

    def s3(self):
        self.to_across().wait()
        self.b32[...] = self.a32[span(self.at.row, self.h2), :] + self.rx2[...].astype(F32)
        self.b16[...] = self.b32[...].astype(BF16)
        for copy in self.to_parts():
            copy.start()

    def s4(self):
        at = self.at
        whole = self.rx3.at[0:len(self.parts)]
        remote(whole, whole, self.z_s.at[0], self.z_r.at[0], self.parts[0][2]).wait()
        total = self.b32[span(self.mine, self.h3), :]
        for slot, _, _ in self.parts:
            total = total + self.rx3[slot].astype(F32)
        for i, place in enumerate(at.bits):
            self.out_x[i] = total.astype(BF16)
            copy = remote(self.out_x.at[i], self.rx_x.at[i], self.x_s.at[i], self.x_r.at[i], place)
            copy.start()
            copy.wait()
            total = self.out_x[i].astype(F32) + self.rx_x[i].astype(F32)
        self.allg[self.piece(0, at.row), :] = total.astype(BF16)
        for d in at.far:
            self.gather(d).start()
        self.side(0).start()
        self.last(0, 0).start()

    def s5(self):
        for d in self.at.near:
            self.gather(d).wait()
            self.side(d).start()
            self.last(d, 0).start()

    def s6(self):
        for d in [0] + self.at.near:
            self.side(d).wait()
            self.last(d, 1).start()

    def s7(self):
        whole = self.allg.at[0:2 * self.at.bands * self.h3]
        remote(whole, whole, self.f_s.at[0], self.f_r.at[0], self.at.partner).wait()


def split(a):
    high = a.astype(BF16)
    return high, (a - high.astype(F32)).astype(BF16)


def product3(a, b, dims):
    (ah, al), (bh, bl) = split(a), split(b)
    return dot(ah, bh, dims) + (dot(ah, bl, dims) + dot(al, bh, dims))


def identity(rows):
    shape = (rows, rows)
    return (lax.broadcasted_iota(jnp.int32, shape, 0)
            == lax.broadcasted_iota(jnp.int32, shape, 1)).astype(F32)


def factor_tile(d_ref, t_ref, hooks):
    G, SUB, BLK = 32, 8, 16
    H, K = G // SUB, BLK // SUB
    sub = lax.broadcasted_iota(jnp.int32, (SUB, TILE), 0)

    def spread(block, i):
        return jnp.broadcast_to(block[i:i + 1, :], (SUB, TILE))

    def lane(block, c):
        where = jnp.full((SUB, TILE), c, jnp.int32)
        return jnp.take_along_axis(block, where, axis=1, mode="promise_in_bounds")

    def step(g, carry):
        start = g * G if isinstance(g, int) else pl.multiple_of(g * G, G)
        lefts = [d_ref[pl.ds(start + h * SUB, SUB), 0:TILE] for h in range(H)]
        rights = [d_ref[pl.ds(start + h * SUB, SUB), TILE:2 * TILE] for h in range(H)]
        us, vs = [None] * H, [None] * H
        for b in range(G // BLK):
            h0 = b * K
            cols = [{h: lane(lefts[h], start + (b * BLK + c)) for h in range(h0 + c // SUB, H)}
                    for c in range(BLK)]
            pivot = spread(cols[0][h0], 0)
            for j in range(BLK):
                k, i = h0 + j // SUB, j % SUB
                r = lax.rsqrt(pivot)
                low = {c: spread(cols[j][h0 + c // SUB], c % SUB) for c in range(j + 1, BLK)}
                if j + 1 < BLK:
                    low[j + 1] = low[j + 1] * r
                    pivot = spread(cols[j + 1][h0 + (j + 1) // SUB], (j + 1) % SUB) - low[j + 1] * low[j + 1]
                for h in range(k, H):
                    cols[j][h] = cols[j][h] * r
                u, v = spread(lefts[k], i) * r, spread(rights[k], i) * r
                us[k] = u if i == 0 else jnp.where(sub == i, u, us[k])
                vs[k] = v if i == 0 else jnp.where(sub == i, v, vs[k])
                for c in range(j + 1, BLK):
                    scaled = low[c] if c == j + 1 else low[c] * r
                    for h in range(h0 + c // SUB, H):
                        cols[c][h] = cols[c][h] - cols[j][h] * scaled
                for h in range(k if i < SUB - 1 else k + 1, H):
                    lefts[h] = lefts[h] - cols[j][h] * u
                    rights[h] = rights[h] - cols[j][h] * v
        u_all = jnp.concatenate(us, axis=0)
        v_all = jnp.concatenate(vs, axis=0)
        t_ref[pl.ds(start, G), :] = v_all
        if isinstance(g, int):
            for stage in hooks[g]:
                stage()
            return carry
        both = jnp.concatenate([u_all, v_all], axis=1)
        high = both.astype(BF16).astype(F32)
        low = both - high
        lhs = jnp.concatenate([high[:, :TILE], high[:, :TILE], low[:, :TILE]], axis=0)
        rhs = jnp.concatenate([high, low, high], axis=0)
        d_ref[...] -= dot(lhs.astype(BF16), rhs.astype(BF16), ((0,), (0,)))
        for k, stages in enumerate(hooks[:-1]):
            if stages:
                @pl.when(g == k)
                def _():
                    for stage in stages:
                        stage()
        return carry

    lax.fori_loop(0, TILE // G - 1, step, 0)
    step(TILE // G - 1, 0)


def ace_kernel(bands, groups, orb, kern, blk, ace, exch, full, extra, w, wx, a, rest, x16, xlow, mba,
               d_ref, t_ref, proj, proj2, bfull, acc, applied, applied2, back, loc, m_s, m_r, n_s, n_r, c_s, c_r,
               d_s, d_r, b_s, b_r, p_s, p_r, t_s, e_s, e_r, f_s, f_r, *scratch):
    at = Place(bands, groups)
    me, team = at.me, at.team
    own, bown = ace.shape[0], exch.shape[0]
    cols = w.shape[1]
    n, nblk = own * bands, bown * bands
    n2 = n // 2
    scale = 1.0 / (ace.shape[1] * groups)
    inner = Reduce(at, scratch[:SCRATCH], True)
    cross = Reduce(at, scratch[SCRATCH:2 * SCRATCH], False)
    couple = Reduce(at, scratch[2 * SCRATCH:], False)
    greet(at.everyone())

    def chunk(index):
        return pl.ds(pl.multiple_of(index * cols, TILE), cols)

    def twin(index):
        return chunk(lax.rem(index + team, bands))

    mine = full.at[span(me, own)]
    also = extra.at[span(me, own)]
    bmine = bfull.at[span(me, bown)]

    def kept():
        return [pltpu.make_async_copy(orb.at[:, chunk(me)], mine, loc.at[0]),
                pltpu.make_async_copy(orb.at[:, twin(me)], also, loc.at[1])]

    def to_mates():
        copies = []
        for j in range(1, team):
            p = at.half * team + at.mate(j)
            copies.append(remote(orb.at[:, chunk(p)], mine, m_s.at[j], m_r.at[j], {"band": p}))
            copies.append(remote(orb.at[:, twin(p)], also, n_s.at[j], n_r.at[j], {"band": p}))
        return copies

    def to_rival(t, sender):
        p = at.rival(t)
        return remote(orb.at[:, chunk(p)], mine, c_s.at[t], c_r.at[sender], {"band": p})

    parts = [(0, cols // 2 // LANES * LANES), (cols // 2 // LANES * LANES, cols)]
    parts = [part for part in parts if part[0] < part[1]]

    def twin_rival(t, sender, lo, hi):
        p = at.rival(t)
        first = pl.multiple_of(lax.rem(p + team, bands) * cols + lo, TILE)
        k = 0 if hi <= parts[0][1] else 1
        return remote(orb.at[:, pl.ds(first, hi - lo)], extra.at[span(me, own), lo:hi],
                      d_s.at[t, k], d_r.at[sender, k], {"band": p})

    slices = [(t, lo) for t in reversed(range(team)) for lo in range(0, cols, LANES)]
    left = {True: list(slices), False: list(slices)}
    near = at.rank >= team // 2

    def upward(count, first=True):
        batch, left[first][:] = left[first][:count], left[first][count:]

        def go():
            @pl.when((at.half == 0) & (near if first else ~near))
            def _():
                for t, lo in batch:
                    twin_rival(t, at.rank, lo, lo + LANES).start()
        return go

    def block(slot, p, sender):
        return remote(blk.at[:, chunk(p)], bmine, b_s.at[slot], b_r.at[sender], {"band": p})

    def block_rival(t):
        return lambda: block(t, at.rival(t), me).start()

    def block_mates():
        for j in range(1, team):
            block(team + j, at.half * team + at.mate(j), me).start()

    def bkept():
        return pltpu.make_async_copy(blk.at[:, chunk(me)], bmine, loc.at[2])

    for copy in to_mates():
        copy.start()
    for t in range(team):
        to_rival(t, at.rank).start()
    for copy in kept():
        copy.start()
    bkept().start()

    def weigh(rows, columns):
        return (-(rows.astype(F32) * kern[:, columns])).astype(BF16)

    for copy in kept() + to_mates():
        copy.wait()
    band = span(at.half, n2)
    w[band, :] = weigh(full[band, :], chunk(me))
    wx[band, :] = weigh(extra[band, :], twin(me))
    row = 0
    for s in range(0, n2, TILE):
        e = s + TILE
        product = (dot(w[span(at.half, TILE, s, n2), :], full[span(at.half, e, 0, n2), :],
                       ((1,), (1,)))
                   + dot(wx[span(at.half, TILE, s, n2), :], extra[span(at.half, e, 0, n2), :],
                         ((1,), (1,))))
        for c in range(0, e, TILE):
            inner.put(row, product[:, c:c + TILE])
            row += TILE
    inner.pad(row)
    inner.s1()
    inner.s2()
    inner.s3()
    inner.s4()
    for t in range(team):
        to_rival(t, t).wait_recv()
    other = span(1 - at.half, n2)
    w[other, :] = weigh(full[other, :], chunk(me))
    row = 0
    for s in range(n2, n, TILE):
        product = dot(w[s:s + TILE, :], full[0:n2, :], ((1,), (1,)))
        for c in range(0, n2, TILE):
            cross.put(row, product[:, c:c + TILE])
            row += TILE
    cross.pad(row)
    cross.s1()
    for t in range(team - 1):
        block_rival(t)()
    cross.s2()
    inner.s5()
    cross.s3()
    block_rival(team - 1)()
    block_mates()
    inner.s6()
    inner.s7()
    row = 0
    for base in (0, n2):
        for s in range(base, base + n2, TILE):
            for c in range(base, s + TILE, TILE):
                a[s:s + TILE, c:c + TILE] = inner.allg[row:row + TILE, :].astype(F32) * -scale
                row += TILE
        row = inner.rows
    rest[...] = identity(n)
    x16[...] = jnp.zeros_like(x16)
    xlow[...] = jnp.zeros_like(xlow)

    def couple_start():
        bkept().wait()
        for d in range(1, bands):
            block(d, at.peer[d], at.peer[d]).wait_recv()
        half = nblk // 2
        for h in range(2):
            couple.put(h * n, dot(w[...], bfull[h * half:(h + 1) * half, :], ((1,), (1,))))
        couple.s1()

    cuts = sorted(set(range(0, n, TILE)) | set(range(0, n, own)) | {n})
    pieces = list(enumerate(zip(cuts[:-1], cuts[1:])))

    def piece(q, r0, r1, source, target, other):
        lo = r0 % own
        if other:
            return strip(q, r0, r1, source, target, 0, 0, cols)
        return remote(proj.at[r0:r1], ace.at[lo:lo + r1 - r0, chunk(source)],
                      p_s.at[0], p_r.at[0], {"band": target})

    def stay(q, r0, r1, other):
        lo = r0 % own
        if other:
            return strip_stay(q, r0, r1, 0, 0, cols)
        return pltpu.make_async_copy(
            proj.at[r0:r1], ace.at[lo:lo + r1 - r0, chunk(me)], t_s.at[0])

    def some(source, c0, c1):
        first = lax.rem(source + team, bands) * cols + c0
        return pl.ds(pl.multiple_of(first, TILE), c1 - c0)

    def strip(q, r0, r1, source, target, k, c0, c1):
        lo = r0 % own
        return remote(proj2.at[r0:r1, c0:c1], ace.at[lo:lo + r1 - r0, some(source, c0, c1)],
                      p_s.at[0], p_r.at[0], {"band": target})

    def strip_stay(q, r0, r1, k, c0, c1):
        lo = r0 % own
        return pltpu.make_async_copy(
            proj2.at[r0:r1, c0:c1], ace.at[lo:lo + r1 - r0, some(me, c0, c1)], t_s.at[0])

    def deliver(lo, hi, other):
        for q, (r0, r1) in pieces:
            if lo <= r0 < hi:
                owner = r0 // own

                @pl.when((me != owner) & (at.half == owner // team))
                def _():
                    piece(q, r0, r1, me, owner, other).start()

                @pl.when(me == owner)
                def _():
                    stay(q, r0, r1, other).start()

    def project(lo, hi, c0, c1):
        proj2[lo:hi, c0:c1] = (dot(x16[lo:hi, 0:hi], wx[0:hi, c0:c1], ((1,), (0,)))
                               + dot(xlow[lo:hi, 0:hi], wx[0:hi, c0:c1], ((1,), (0,)))).astype(BF16)

    def spare():
        @pl.when(at.half == 0)
        def _():
            project(0, n2, 0, cols)

        deliver(0, n2, 1)

    tiles = n2 // TILE
    hooks = [[[] for _ in range(4)] for _ in range(2 * tiles)]

    def at_hook(k, g, *stages):
        hooks[k][g] += stages

    at_hook(0, 2, cross.s4)
    at_hook(tiles - 2, 0, couple_start)
    at_hook(tiles - 2, 2, cross.s5, couple.s2)
    at_hook(tiles - 2, 3, upward(1), upward(1, False))
    at_hook(tiles - 1, 0, upward(1), upward(1, False))
    at_hook(tiles - 1, 1, upward(1))
    at_hook(tiles - 1, 2, cross.s6)
    closing = upward(3)
    at_hook(tiles, 1, couple.s4, lambda: deliver(0, n2, 0), upward(len(slices)))
    at_hook(tiles + 1, 0, upward(len(slices), False))
    at_hook(tiles + 1, 2, couple.s5, spare)
    at_hook(tiles + 2, 1, couple.s6)
    at_hook(tiles + 2, 3, couple.s7)

    def attach(lo, hi):
        half = nblk // 2
        for h in range(2):
            part = allg_dot(lo, hi, h) * scale
            update = dot(part.astype(BF16), proj[lo:hi, :], ((0,), (0,)))
            if lo == 0:
                acc[h * half:(h + 1) * half, :] = update
            else:
                acc[h * half:(h + 1) * half, :] += update

    def allg_dot(lo, hi, h):
        return dot(x16[lo:hi, 0:hi], couple.allg[h * n:h * n + hi, :], ((1,), (0,)))

    for k, s in enumerate(range(0, n, TILE)):
        e = s + TILE
        top = n2 if s < n2 else n
        d_ref[:, 0:TILE] = a[s:e, s:e]
        d_ref[:, TILE:] = identity(TILE)
        factor_tile(d_ref, t_ref, hooks[k])
        tile = t_ref[...]
        rows = product3(tile, rest[s:e, 0:e], ((1,), (0,)))
        high, low = split(rows)
        x16[s:e, 0:e] = high
        xlow[s:e, 0:e] = low
        proj[s:e, :] = (dot(high, w[0:e, :], ((1,), (0,)))
                        + dot(low, w[0:e, :], ((1,), (0,)))).astype(BF16)
        if s >= n2:
            deliver(s, e, 0)
        if e < top:
            panel = product3(a[e:top, s:e], tile, ((1,), (1,)))
            for c in range(e, top, TILE):
                a[c:top, c:c + TILE] -= product3(panel[c - e:], panel[c - e:c - s], ((1,), (1,)))
            rest[e:top, 0:e] -= product3(panel, rows, ((1,), (0,)))
        if e == n2:
            cross.s7()
            row = 0
            for r in range(0, n2, TILE):
                for c in range(0, n2, TILE):
                    mba[r:r + TILE, c:c + TILE] = cross.allg[row:row + TILE, :]
                    row += TILE
            both = (((1,), (1,)))
            below = (dot(mba[...], x16[0:n2, 0:n2], both) + dot(mba[...], xlow[0:n2, 0:n2], both)) * -scale
            bh, bl = split(below)
            for c in range(0, n2, TILE):
                d = c + TILE
                a[n2 + c:n, n2 + c:n2 + d] -= (
                    dot(bh[c:], bh[c:d], both) + (dot(bh[c:], bl[c:d], both) + dot(bl[c:], bh[c:d], both)))
            over = ((1,), (0,))
            xh = x16[0:n2, 0:n2]
            couple.s3()
            closing()
            rest[n2:, 0:n2] = -(dot(bh, xh, over) + (dot(bh, xlow[0:n2, 0:n2], over) + dot(bl, xh, over)))
    attach(0, n)
    applied[...] = (-acc[...]).astype(BF16)

    def out(slot, p, sender):
        return remote(applied.at[span(p, bown)], exch.at[:, chunk(sender)],
                      e_s.at[slot], e_r.at[sender], {"band": p})

    def out2(slot, p, sender):
        return remote(applied2.at[span(lax.rem(p, team), bown)], exch.at[:, twin(sender)],
                      f_s.at[slot], f_r.at[sender], {"band": p})

    def held():
        return pltpu.make_async_copy(applied.at[span(me, bown)], exch.at[:, chunk(me)], loc.at[3])

    def held2():
        return pltpu.make_async_copy(applied2.at[span(at.rank, bown)], exch.at[:, twin(me)], loc.at[4])

    mates = [at.half * team + at.mate(j) for j in range(1, team)]

    @pl.when(at.half == 1)
    def _():
        for t in range(team):
            out(t, at.rival(t), me).start()

    for j, p in enumerate(mates):
        out(team + j, p, me).start()
    held().start()

    @pl.when(at.half == 1)
    def _():
        turned = ((0,), (0,))
        part = dot(x16[...], couple.allg[n:2 * n, :], ((1,), (0,))) * -scale
        ph, pq = split(part)
        back[...] = (dot(ph, x16[...], turned)
                     + (dot(ph, xlow[...], turned) + dot(pq, x16[...], turned)))

    @pl.when(at.half == 1)
    def _():
        bh, bl = split(back[...])
        forth = ((1,), (0,))
        for k, (c0, c1) in enumerate(parts):
            for t in range(team):
                twin_rival(t, t, c0, c1).wait_recv()
            wx[0:n2, c0:c1] = (-(extra[0:n2, c0:c1].astype(F32) * kern[:, some(me, c0, c1)])).astype(BF16)
            project(n2, n, c0, c1)
            for q, (r0, r1) in pieces:
                if r0 >= n2:
                    owner = r0 // own

                    @pl.when(me != owner)
                    def _():
                        strip(q, r0, r1, me, owner, k, c0, c1).start()

                    @pl.when(me == owner)
                    def _():
                        strip_stay(q, r0, r1, k, c0, c1).start()

            applied2[:, c0:c1] = (dot(bh, wx[:, c0:c1], forth) + dot(bl, wx[:, c0:c1], forth)).astype(BF16)
        for j, p in enumerate(mates):
            out2(j, p, me).start()
        held2().start()

    for t in range(team):
        to_rival(t, t).wait_send()
        block(t, me, me).wait_send()
    for j in range(1, team):
        block(team + j, me, me).wait_send()

    @pl.when(at.half == 0)
    def _():
        for t in range(team):
            for c0, c1 in parts:
                twin_rival(t, t, c0, c1).wait_send()

    everything = ace.at[:, 0:2 * cols * (team - 1)]
    remote(everything, everything, p_s.at[0], p_r.at[0], {"band": mates[0]}).wait()
    local = ace.at[:, 0:2 * cols]
    pltpu.make_async_copy(local, local, t_s.at[0]).wait()
    for j, p in enumerate(mates):
        out(team + j, p, p).wait()
    held().wait()

    @pl.when(at.half == 1)
    def _():
        for t in range(team):
            out(t, at.rival(t), me).wait_send()
        for j, p in enumerate(mates):
            out2(j, p, p).wait()
        held2().wait()

    @pl.when(at.half == 0)
    def _():
        for t in range(team):
            out(t, me, at.rival(t)).wait_recv()


def shards(orbitals, kernel, block_vectors):
    groups, bands = lax.axis_size("ga"), lax.axis_size("band")
    own, width = orbitals.shape
    bown = block_vectors.shape[0]
    cols = width // bands
    n, nblk = own * bands, bown * bands
    n2, team = n // 2, bands // 2
    levels = max(groups.bit_length() - 3, 1)
    tiles = n2 // TILE

    def padded(rows, parts):
        unit = 4 * parts * 16
        return -(-rows // unit) * unit

    vmem, hbm = pl.BlockSpec(memory_space=pltpu.VMEM), pl.BlockSpec(memory_space=pl.ANY)
    dma = pltpu.SemaphoreType.DMA
    many, some = dma((bands,)), dma((team,))
    return pl.pallas_call(
        functools.partial(ace_kernel, bands, groups),
        name="ace",
        out_shape=(
            jax.ShapeDtypeStruct((own, width), BF16),
            jax.ShapeDtypeStruct((bown, width), BF16),
        ),
        in_specs=[hbm, vmem, hbm],
        out_specs=(hbm, hbm),
        scratch_shapes=[
            pltpu.VMEM((n, cols), BF16),
            pltpu.VMEM((n, cols), BF16),
            pltpu.VMEM((n, cols), BF16),
            pltpu.VMEM((n, cols), BF16),
            pltpu.VMEM((n, n), F32),
            pltpu.VMEM((n, n), F32),
            pltpu.VMEM((n, n), BF16),
            pltpu.VMEM((n, n), BF16),
            pltpu.VMEM((n2, n2), BF16),
            pltpu.VMEM((TILE, 2 * TILE), F32),
            pltpu.VMEM((TILE, TILE), F32),
            pltpu.VMEM((n, cols), BF16),
            pltpu.VMEM((n, cols), BF16),
            pltpu.VMEM((nblk, cols), BF16),
            pltpu.VMEM((nblk, cols), F32),
            pltpu.VMEM((nblk, cols), BF16),
            pltpu.VMEM((nblk // 2, cols), BF16),
            pltpu.VMEM((nblk // 2, n), F32),
            dma((5,)), some, some, some, some, some, some, dma((team, 2)), dma((team, 2)),
            many, many, dma((1,)), dma((1,)), dma((1,)),
            many, many, many, many,
        ]
        + reduce_scratch(padded(tiles * (tiles + 1) // 2 * TILE, team), team, bands, levels, 2)
        + reduce_scratch(padded(tiles * tiles * TILE, bands), bands, bands, levels, 1)
        + reduce_scratch(2 * n, bands, bands, levels, 1),
        compiler_params=pltpu.CompilerParams(
            collective_id=0, has_side_effects=True, vmem_limit_bytes=56 * 2**20),
    )(orbitals, kernel.reshape(1, width), block_vectors)


def solution(mesh):
    placed = (P(("img", "band"), "ga"), P("ga"), P(("img", "band"), "ga"))
    return jax.shard_map(
        shards,
        mesh=mesh,
        in_specs=placed,
        out_specs=(P(("img", "band"), "ga"), P(("img", "band"), "ga")),
        check_vma=False,
    )
```

```python
import functools

import jax
import jax.numpy as jnp
from jax import lax
from jax.experimental import pallas as pl
from jax.experimental.pallas import tpu as pltpu
from jax.sharding import PartitionSpec as P

MESH = pl.DeviceIdType.MESH
F32 = jnp.float32
BF16 = jnp.bfloat16
TILE = 128
LANES = 128


def remote(src, dst, send_sem, recv_sem, where):
    return pltpu.make_async_remote_copy(
        src_ref=src, dst_ref=dst, send_sem=send_sem, recv_sem=recv_sem,
        device_id=where, device_id_type=MESH,
    )


def greet(places):
    barrier = pltpu.get_barrier_semaphore()
    for place in places:
        pl.semaphore_signal(barrier, inc=1, device_id=place, device_id_type=MESH)
    pl.semaphore_wait(barrier, len(places))


def dot(a, b, dims):
    return lax.dot_general(a, b, (dims, ((), ())), preferred_element_type=F32)


class Place:
    def __init__(self, bands, groups):
        self.bands = bands
        self.me = lax.axis_index("band")
        self.team = bands // 2
        self.half = self.me // self.team
        self.rank = lax.rem(self.me, self.team)
        ga = lax.axis_index("ga")
        self.core = lax.rem(ga, 2)
        self.row = lax.rem(ga // 2, 2)
        self.partner = {"ga": ga + 1 - 2 * self.core}
        self.across = {"ga": ga + 2 - 4 * self.row}
        self.peer = [lax.rem(self.me + d, bands) for d in range(bands)]
        self.far = sorted(range(1, bands), key=lambda d: -min(d, bands - d))
        self.near = self.far[::-1]
        self.bits = []
        stride = 4
        while stride < groups:
            self.bits.append({"ga": ga + stride * (1 - 2 * lax.rem(ga // stride, 2))})
            stride *= 2

    def band(self, d):
        return {"band": self.peer[d]}

    def mate(self, j):
        return lax.rem(self.rank + j, self.team)

    def rival(self, t):
        return (1 - self.half) * (self.team + t) + self.half * (self.team - 1 - t)

    def everyone(self):
        return [self.band(d) for d in range(1, self.bands)] + [self.partner, self.across] + self.bits


def span(index, size, offset=0, stride=None):
    return pl.ds(pl.multiple_of(offset + index * (stride or size), 16), size)


def reduce_scratch(rows, parts, bands, levels, sides):
    h1, h2 = rows // 2, rows // 4
    h3 = h2 // parts
    dma = pltpu.SemaphoreType.DMA
    shapes = [
        ((rows, TILE), F32), ((rows, TILE), BF16), ((h1, TILE), BF16),
        ((h1, TILE), F32), ((h1, TILE), BF16), ((h2, TILE), BF16),
        ((h2, TILE), F32), ((h2, TILE), BF16), ((parts, h3, TILE), BF16),
        ((levels, h3, TILE), BF16), ((levels, h3, TILE), BF16), ((sides * rows, TILE), BF16),
    ]
    return [pltpu.VMEM(*shape) for shape in shapes] + [
        dma((4,)), dma((1,)), dma((1,)), dma((levels,)), dma((levels,)),
        dma((bands,)), dma((bands,)), dma((1,)), dma((1,)),
        dma((1,)), dma((1,)),
    ]


SCRATCH = 23


class Reduce:
    def __init__(self, at, scratch, by_team):
        self.at = at
        (self.p32, self.p16, self.rx1, self.a32, self.a16, self.rx2, self.b32, self.b16, self.rx3,
         self.out_x, self.rx_x, self.allg, self.one, self.z_s, self.z_r, self.x_s, self.x_r,
         self.g_s, self.g_r, self.y_s, self.y_r, self.f_s, self.f_r) = scratch
        self.rows = self.p32.shape[0]
        self.h1, self.h2, self.h3 = self.rx1.shape[0], self.rx2.shape[0], self.rx3.shape[1]
        self.by_team = by_team
        if by_team:
            self.mine = at.rank
            self.parts = [(j, at.mate(j), {"band": at.half * at.team + at.mate(j)})
                          for j in range(1, at.team)]
        else:
            self.mine = at.me
            self.parts = [(d, at.peer[d], at.band(d)) for d in at.far]

    def put(self, row, value):
        size = value.shape[0]
        self.p32[row:row + size, :] = value
        self.p16[row:row + size, :] = value.astype(BF16)

    def pad(self, row):
        size = self.rows - row
        if size:
            self.put(row, jnp.zeros((size, TILE), F32))

    def to_partner(self):
        at = self.at
        return remote(self.p16.at[span(1 - at.core, self.h1)], self.rx1,
                      self.one.at[0], self.one.at[1], at.partner)

    def to_across(self):
        at = self.at
        return remote(self.a16.at[span(1 - at.row, self.h2)], self.rx2,
                      self.one.at[2], self.one.at[3], at.across)

    def to_parts(self):
        return [remote(self.b16.at[span(index, self.h3)], self.rx3.at[slot],
                       self.z_s.at[0], self.z_r.at[0], where)
                for slot, index, where in self.parts]

    def piece(self, d, row):
        at = self.at
        source = lax.rem(at.me + at.bands - d, at.bands)
        offset = at.core * self.h1 + row * self.h2
        if self.by_team:
            offset = offset + (source // at.team) * self.rows
            source = lax.rem(source, at.team)
        return span(source, self.h3, offset)

    def gather(self, d):
        own = self.allg.at[self.piece(0, self.at.row)]
        return remote(own, own, self.g_s.at[d], self.g_r.at[d], self.at.band(d))

    def side(self, d):
        there = self.allg.at[self.piece(d, self.at.row)]
        return remote(there, there, self.y_s.at[0], self.y_r.at[0], self.at.across)

    def last(self, d, other):
        row = 1 - self.at.row if other else self.at.row
        there = self.allg.at[self.piece(d, row)]
        return remote(there, there, self.f_s.at[0], self.f_r.at[0], self.at.partner)

    def s1(self):
        self.to_partner().start()

    def s2(self):
        self.to_partner().wait()
        self.a32[...] = self.p32[span(self.at.core, self.h1), :] + self.rx1[...].astype(F32)
        self.a16[...] = self.a32[...].astype(BF16)
        self.to_across().start()

    def s3(self):
        self.to_across().wait()
        self.b32[...] = self.a32[span(self.at.row, self.h2), :] + self.rx2[...].astype(F32)
        self.b16[...] = self.b32[...].astype(BF16)
        for copy in self.to_parts():
            copy.start()

    def s4(self):
        at = self.at
        whole = self.rx3.at[0:len(self.parts)]
        remote(whole, whole, self.z_s.at[0], self.z_r.at[0], self.parts[0][2]).wait()
        total = self.b32[span(self.mine, self.h3), :]
        for slot, _, _ in self.parts:
            total = total + self.rx3[slot].astype(F32)
        for i, place in enumerate(at.bits):
            self.out_x[i] = total.astype(BF16)
            copy = remote(self.out_x.at[i], self.rx_x.at[i], self.x_s.at[i], self.x_r.at[i], place)
            copy.start()
            copy.wait()
            total = self.out_x[i].astype(F32) + self.rx_x[i].astype(F32)
        self.allg[self.piece(0, at.row), :] = total.astype(BF16)
        for d in at.far:
            self.gather(d).start()
        self.side(0).start()
        self.last(0, 0).start()

    def s5(self):
        for d in self.at.near:
            self.gather(d).wait()
            self.side(d).start()
            self.last(d, 0).start()

    def s6(self):
        whole = self.allg.at[0:self.at.bands * self.h3]
        remote(whole, whole, self.y_s.at[0], self.y_r.at[0], self.at.across).wait()
        for d in [0] + self.at.near:
            self.last(d, 1).start()

    def s7(self):
        whole = self.allg.at[0:2 * self.at.bands * self.h3]
        remote(whole, whole, self.f_s.at[0], self.f_r.at[0], self.at.partner).wait()


def split(a):
    high = a.astype(BF16)
    return high, (a - high.astype(F32)).astype(BF16)


def product3(a, b, dims):
    (ah, al), (bh, bl) = split(a), split(b)
    return dot(ah, bh, dims) + (dot(ah, bl, dims) + dot(al, bh, dims))


def identity(rows):
    shape = (rows, rows)
    return (lax.broadcasted_iota(jnp.int32, shape, 0)
            == lax.broadcasted_iota(jnp.int32, shape, 1)).astype(F32)


def factor_tile(d_ref, t_ref, hooks):
    G, SUB, BLK = 32, 8, 16
    H, K = G // SUB, BLK // SUB
    sub = lax.broadcasted_iota(jnp.int32, (SUB, TILE), 0)

    def spread(block, i):
        return jnp.broadcast_to(block[i:i + 1, :], (SUB, TILE))

    def lane(block, c):
        where = jnp.full((SUB, TILE), c, jnp.int32)
        return jnp.take_along_axis(block, where, axis=1, mode="promise_in_bounds")

    def step(g, carry):
        start = g * G if isinstance(g, int) else pl.multiple_of(g * G, G)
        lefts = [d_ref[pl.ds(start + h * SUB, SUB), 0:TILE] for h in range(H)]
        rights = [d_ref[pl.ds(start + h * SUB, SUB), TILE:2 * TILE] for h in range(H)]
        us, vs = [None] * H, [None] * H
        for b in range(G // BLK):
            h0 = b * K
            cols = [{h: lane(lefts[h], start + (b * BLK + c)) for h in range(h0 + c // SUB, H)}
                    for c in range(BLK)]
            pivot = spread(cols[0][h0], 0)
            for j in range(BLK):
                k, i = h0 + j // SUB, j % SUB
                r = lax.rsqrt(pivot)
                low = {c: spread(cols[j][h0 + c // SUB], c % SUB) for c in range(j + 1, BLK)}
                if j + 1 < BLK:
                    low[j + 1] = low[j + 1] * r
                    pivot = spread(cols[j + 1][h0 + (j + 1) // SUB], (j + 1) % SUB) - low[j + 1] * low[j + 1]
                for h in range(k, H):
                    cols[j][h] = cols[j][h] * r
                u, v = spread(lefts[k], i) * r, spread(rights[k], i) * r
                us[k] = u if i == 0 else jnp.where(sub == i, u, us[k])
                vs[k] = v if i == 0 else jnp.where(sub == i, v, vs[k])
                for c in range(j + 1, BLK):
                    scaled = low[c] if c == j + 1 else low[c] * r
                    for h in range(h0 + c // SUB, H):
                        cols[c][h] = cols[c][h] - cols[j][h] * scaled
                for h in range(k if i < SUB - 1 else k + 1, H):
                    lefts[h] = lefts[h] - cols[j][h] * u
                    rights[h] = rights[h] - cols[j][h] * v
        u_all = jnp.concatenate(us, axis=0)
        v_all = jnp.concatenate(vs, axis=0)
        t_ref[pl.ds(start, G), :] = v_all
        if isinstance(g, int):
            for stage in hooks[g]:
                stage()
            return carry
        both = jnp.concatenate([u_all, v_all], axis=1)
        high = both.astype(BF16).astype(F32)
        low = both - high
        lhs = jnp.concatenate([high[:, :TILE], high[:, :TILE], low[:, :TILE]], axis=0)
        rhs = jnp.concatenate([high, low, high], axis=0)
        d_ref[...] -= dot(lhs.astype(BF16), rhs.astype(BF16), ((0,), (0,)))
        for k, stages in enumerate(hooks[:-1]):
            if stages:
                @pl.when(g == k)
                def _():
                    for stage in stages:
                        stage()
        return carry

    lax.fori_loop(0, TILE // G - 1, step, 0)
    step(TILE // G - 1, 0)


def ace_kernel(bands, groups, orb, kern_in, blk, ace, exch, kern, full, extra, w, wx, a, rest, x16, xlow, mba,
               d_ref, t_ref, proj, proj2, bfull, acc, applied, applied2, back, loc, m_s, m_r, n_s, n_r, c_s, c_r,
               d_s, d_r, b_s, b_r, p_s, p_r, t_s, e_s, e_r, f_s, f_r, *scratch):
    at = Place(bands, groups)
    me, team = at.me, at.team
    own, bown = ace.shape[0], exch.shape[0]
    cols = w.shape[1]
    n, nblk = own * bands, bown * bands
    n2 = n // 2
    scale = 1.0 / (ace.shape[1] * groups)
    inner = Reduce(at, scratch[:SCRATCH], True)
    cross = Reduce(at, scratch[SCRATCH:2 * SCRATCH], False)
    couple = Reduce(at, scratch[2 * SCRATCH:], False)
    greet(at.everyone())

    def chunk(index):
        return pl.ds(pl.multiple_of(index * cols, TILE), cols)

    def twin(index):
        return chunk(lax.rem(index + team, bands))

    mine = full.at[span(me, own)]
    also = extra.at[span(me, own)]
    bmine = bfull.at[span(me, bown)]

    def kept():
        return [pltpu.make_async_copy(orb.at[:, chunk(me)], mine, loc.at[0]),
                pltpu.make_async_copy(orb.at[:, twin(me)], also, loc.at[1]),
                pltpu.make_async_copy(kern_in, kern, loc.at[5])]

    def to_mates():
        copies = []
        for j in range(1, team):
            p = at.half * team + at.mate(j)
            copies.append(remote(orb.at[:, chunk(p)], mine, m_s.at[j], m_r.at[j], {"band": p}))
            copies.append(remote(orb.at[:, twin(p)], also, n_s.at[j], n_r.at[j], {"band": p}))
        return copies

    def to_rival(t, sender):
        p = at.rival(t)
        return remote(orb.at[:, chunk(p)], mine, c_s.at[t], c_r.at[sender], {"band": p})

    parts = [(0, cols // 2 // LANES * LANES), (cols // 2 // LANES * LANES, cols)]
    parts = [part for part in parts if part[0] < part[1]]

    def twin_rival(t, sender, lo, hi):
        p = at.rival(t)
        first = pl.multiple_of(lax.rem(p + team, bands) * cols + lo, TILE)
        k = 0 if hi <= parts[0][1] else 1
        return remote(orb.at[:, pl.ds(first, hi - lo)], extra.at[span(me, own), lo:hi],
                      d_s.at[t, k], d_r.at[sender, k], {"band": p})

    slices = [(t, lo) for t in reversed(range(team)) for lo in range(0, cols, LANES)]
    left = {True: list(slices), False: list(slices)}
    near = at.rank >= team // 2

    def upward(count, first=True):
        batch, left[first][:] = left[first][:count], left[first][count:]

        def go():
            @pl.when((at.half == 0) & (near if first else ~near))
            def _():
                for t, lo in batch:
                    twin_rival(t, at.rank, lo, lo + LANES).start()
        return go

    def block(slot, p, sender):
        return remote(blk.at[:, chunk(p)], bmine, b_s.at[slot], b_r.at[sender], {"band": p})

    def block_rival(t):
        return lambda: block(t, at.rival(t), me).start()

    def block_mates():
        for j in range(1, team):
            block(team + j, at.half * team + at.mate(j), me).start()

    def bkept():
        return pltpu.make_async_copy(blk.at[:, chunk(me)], bmine, loc.at[2])

    for copy in to_mates():
        copy.start()
    for t in range(team):
        to_rival(t, at.rank).start()
    for copy in kept():
        copy.start()
    bkept().start()

    def weigh(rows, columns):
        return (-(rows.astype(F32) * kern[:, columns])).astype(BF16)

    for copy in kept() + to_mates():
        copy.wait()
    band = span(at.half, n2)
    w[band, :] = weigh(full[band, :], chunk(me))
    wx[band, :] = weigh(extra[band, :], twin(me))
    row = 0
    for s in range(0, n2, TILE):
        e = s + TILE
        product = (dot(w[span(at.half, TILE, s, n2), :], full[span(at.half, e, 0, n2), :],
                       ((1,), (1,)))
                   + dot(wx[span(at.half, TILE, s, n2), :], extra[span(at.half, e, 0, n2), :],
                         ((1,), (1,))))
        for c in range(0, e, TILE):
            inner.put(row, product[:, c:c + TILE])
            row += TILE
    inner.pad(row)
    inner.s1()
    inner.s2()
    inner.s3()
    for t in range(team):
        to_rival(t, t).wait_recv()
    other = span(1 - at.half, n2)
    w[other, :] = weigh(full[other, :], chunk(me))
    row = 0
    for s in range(n2, n, TILE):
        product = dot(w[s:s + TILE, :], full[0:n2, :], ((1,), (1,)))
        for c in range(0, n2, TILE):
            cross.put(row, product[:, c:c + TILE])
            row += TILE
    cross.pad(row)
    cross.s1()
    inner.s4()
    for t in range(team - 1):
        block_rival(t)()
    cross.s2()
    inner.s5()
    cross.s3()
    block_rival(team - 1)()
    block_mates()
    inner.s6()
    inner.s7()
    row = 0
    for base in (0, n2):
        for s in range(base, base + n2, TILE):
            for c in range(base, s + TILE, TILE):
                a[s:s + TILE, c:c + TILE] = inner.allg[row:row + TILE, :].astype(F32) * -scale
                row += TILE
        row = inner.rows
    rest[...] = identity(n)
    x16[...] = jnp.zeros_like(x16)
    xlow[...] = jnp.zeros_like(xlow)

    def couple_start():
        bkept().wait()
        for d in range(1, bands):
            block(d, at.peer[d], at.peer[d]).wait_recv()
        half = nblk // 2
        for h in range(2):
            couple.put(h * n, dot(w[...], bfull[h * half:(h + 1) * half, :], ((1,), (1,))))
        couple.s1()

    cuts = sorted(set(range(0, n, TILE)) | set(range(0, n, own)) | {n})
    pieces = list(enumerate(zip(cuts[:-1], cuts[1:])))

    def piece(q, r0, r1, source, target, other):
        lo = r0 % own
        if other:
            return strip(q, r0, r1, source, target, 0, 0, cols)
        return remote(proj.at[r0:r1], ace.at[lo:lo + r1 - r0, chunk(source)],
                      p_s.at[0], p_r.at[0], {"band": target})

    def stay(q, r0, r1, other):
        lo = r0 % own
        if other:
            return strip_stay(q, r0, r1, 0, 0, cols)
        return pltpu.make_async_copy(
            proj.at[r0:r1], ace.at[lo:lo + r1 - r0, chunk(me)], t_s.at[0])

    def some(source, c0, c1):
        first = lax.rem(source + team, bands) * cols + c0
        return pl.ds(pl.multiple_of(first, TILE), c1 - c0)

    def strip(q, r0, r1, source, target, k, c0, c1):
        lo = r0 % own
        return remote(proj2.at[r0:r1, c0:c1], ace.at[lo:lo + r1 - r0, some(source, c0, c1)],
                      p_s.at[0], p_r.at[0], {"band": target})

    def strip_stay(q, r0, r1, k, c0, c1):
        lo = r0 % own
        return pltpu.make_async_copy(
            proj2.at[r0:r1, c0:c1], ace.at[lo:lo + r1 - r0, some(me, c0, c1)], t_s.at[0])

    def deliver(lo, hi, other):
        for q, (r0, r1) in pieces:
            if lo <= r0 < hi:
                owner = r0 // own

                @pl.when((me != owner) & (at.half == owner // team))
                def _():
                    piece(q, r0, r1, me, owner, other).start()

                @pl.when(me == owner)
                def _():
                    stay(q, r0, r1, other).start()

    def project(lo, hi, c0, c1):
        proj2[lo:hi, c0:c1] = (dot(x16[lo:hi, 0:hi], wx[0:hi, c0:c1], ((1,), (0,)))
                               + dot(xlow[lo:hi, 0:hi], wx[0:hi, c0:c1], ((1,), (0,)))).astype(BF16)

    def spare():
        @pl.when(at.half == 0)
        def _():
            project(0, n2, 0, cols)

        deliver(0, n2, 1)

    tiles = n2 // TILE
    hooks = [[[] for _ in range(4)] for _ in range(2 * tiles)]

    def at_hook(k, g, *stages):
        hooks[k][g] += stages

    at_hook(0, 1, cross.s4, upward(2))
    at_hook(0, 3, upward(1))
    at_hook(tiles - 2, 0, couple_start)
    at_hook(tiles - 2, 1, cross.s5)
    at_hook(tiles - 2, 2, couple.s2)
    at_hook(tiles - 2, 3, upward(1), upward(1, False))
    at_hook(tiles - 1, 0, upward(1), upward(1, False))
    at_hook(tiles - 1, 1, upward(1))
    at_hook(tiles - 1, 1, cross.s6)
    closing = upward(3)
    at_hook(tiles, 1, couple.s4, lambda: deliver(0, n2, 0), upward(len(slices)))
    at_hook(tiles + 1, 0, upward(len(slices), False))
    at_hook(tiles + 1, 2, couple.s5, spare)
    at_hook(tiles + 2, 1, couple.s6)
    at_hook(tiles + 2, 3, couple.s7)

    def attach(lo, hi):
        half = nblk // 2
        for h in range(2):
            part = allg_dot(lo, hi, h) * scale
            update = dot(part.astype(BF16), proj[lo:hi, :], ((0,), (0,)))
            if lo == 0:
                acc[h * half:(h + 1) * half, :] = update
            else:
                acc[h * half:(h + 1) * half, :] += update

    def allg_dot(lo, hi, h):
        return dot(x16[lo:hi, 0:hi], couple.allg[h * n:h * n + hi, :], ((1,), (0,)))

    for k, s in enumerate(range(0, n, TILE)):
        e = s + TILE
        top = n2 if s < n2 else n
        d_ref[:, 0:TILE] = a[s:e, s:e]
        d_ref[:, TILE:] = identity(TILE)
        factor_tile(d_ref, t_ref, hooks[k])
        tile = t_ref[...]
        rows = product3(tile, rest[s:e, 0:e], ((1,), (0,)))
        high, low = split(rows)
        x16[s:e, 0:e] = high
        xlow[s:e, 0:e] = low
        proj[s:e, :] = (dot(high, w[0:e, :], ((1,), (0,)))
                        + dot(low, w[0:e, :], ((1,), (0,)))).astype(BF16)
        if s >= n2:
            deliver(s, e, 0)
        if e < top:
            panel = product3(a[e:top, s:e], tile, ((1,), (1,)))
            for c in range(e, top, TILE):
                a[c:top, c:c + TILE] -= product3(panel[c - e:], panel[c - e:c - s], ((1,), (1,)))
            rest[e:top, 0:e] -= product3(panel, rows, ((1,), (0,)))
        if e == n2:
            cross.s7()
            row = 0
            for r in range(0, n2, TILE):
                for c in range(0, n2, TILE):
                    mba[r:r + TILE, c:c + TILE] = cross.allg[row:row + TILE, :]
                    row += TILE
            both = (((1,), (1,)))
            below = (dot(mba[...], x16[0:n2, 0:n2], both) + dot(mba[...], xlow[0:n2, 0:n2], both)) * -scale
            bh, bl = split(below)
            for c in range(0, n2, TILE):
                d = c + TILE
                a[n2 + c:n, n2 + c:n2 + d] -= (
                    dot(bh[c:], bh[c:d], both) + (dot(bh[c:], bl[c:d], both) + dot(bl[c:], bh[c:d], both)))
            over = ((1,), (0,))
            xh = x16[0:n2, 0:n2]
            couple.s3()
            closing()
            rest[n2:, 0:n2] = -(dot(bh, xh, over) + (dot(bh, xlow[0:n2, 0:n2], over) + dot(bl, xh, over)))
    attach(0, n)
    applied[...] = (-acc[...]).astype(BF16)

    def out(slot, p, sender):
        return remote(applied.at[span(p, bown)], exch.at[:, chunk(sender)],
                      e_s.at[slot], e_r.at[sender], {"band": p})

    def out2(slot, p, sender):
        return remote(applied2.at[span(lax.rem(p, team), bown)], exch.at[:, twin(sender)],
                      f_s.at[slot], f_r.at[sender], {"band": p})

    def held():
        return pltpu.make_async_copy(applied.at[span(me, bown)], exch.at[:, chunk(me)], loc.at[3])

    def held2():
        return pltpu.make_async_copy(applied2.at[span(at.rank, bown)], exch.at[:, twin(me)], loc.at[4])

    mates = [at.half * team + at.mate(j) for j in range(1, team)]

    @pl.when(at.half == 1)
    def _():
        for t in range(team):
            out(t, at.rival(t), me).start()

    for j, p in enumerate(mates):
        out(team + j, p, me).start()
    held().start()

    @pl.when(at.half == 1)
    def _():
        turned = ((0,), (0,))
        part = dot(x16[...], couple.allg[n:2 * n, :], ((1,), (0,))) * -scale
        ph, pq = split(part)
        back[...] = (dot(ph, x16[...], turned)
                     + (dot(ph, xlow[...], turned) + dot(pq, x16[...], turned)))

    @pl.when(at.half == 1)
    def _():
        bh, bl = split(back[...])
        forth = ((1,), (0,))
        for k, (c0, c1) in enumerate(parts):
            for t in range(team):
                twin_rival(t, t, c0, c1).wait_recv()
            wx[0:n2, c0:c1] = (-(extra[0:n2, c0:c1].astype(F32) * kern[:, some(me, c0, c1)])).astype(BF16)
            project(n2, n, c0, c1)
            for q, (r0, r1) in pieces:
                if r0 >= n2:
                    owner = r0 // own

                    @pl.when(me != owner)
                    def _():
                        strip(q, r0, r1, me, owner, k, c0, c1).start()

                    @pl.when(me == owner)
                    def _():
                        strip_stay(q, r0, r1, k, c0, c1).start()

            applied2[:, c0:c1] = (dot(bh, wx[:, c0:c1], forth) + dot(bl, wx[:, c0:c1], forth)).astype(BF16)
        for j, p in enumerate(mates):
            out2(j, p, me).start()
        held2().start()

    for t in range(team):
        to_rival(t, t).wait_send()
        block(t, me, me).wait_send()
    for j in range(1, team):
        block(team + j, me, me).wait_send()

    @pl.when(at.half == 0)
    def _():
        for t in range(team):
            for c0, c1 in parts:
                twin_rival(t, t, c0, c1).wait_send()

    everything = ace.at[:, 0:2 * cols * (team - 1)]
    remote(everything, everything, p_s.at[0], p_r.at[0], {"band": mates[0]}).wait()
    local = ace.at[:, 0:2 * cols]
    pltpu.make_async_copy(local, local, t_s.at[0]).wait()
    for j, p in enumerate(mates):
        out(team + j, p, p).wait()
    held().wait()

    @pl.when(at.half == 1)
    def _():
        for t in range(team):
            out(t, at.rival(t), me).wait_send()
        for j, p in enumerate(mates):
            out2(j, p, p).wait()
        held2().wait()

    @pl.when(at.half == 0)
    def _():
        for t in range(team):
            out(t, me, at.rival(t)).wait_recv()


def shards(orbitals, kernel, block_vectors):
    groups, bands = lax.axis_size("ga"), lax.axis_size("band")
    own, width = orbitals.shape
    bown = block_vectors.shape[0]
    cols = width // bands
    n, nblk = own * bands, bown * bands
    n2, team = n // 2, bands // 2
    levels = max(groups.bit_length() - 3, 1)
    tiles = n2 // TILE

    def padded(rows, parts):
        unit = 4 * parts * 16
        return -(-rows // unit) * unit

    hbm = pl.BlockSpec(memory_space=pl.ANY)
    dma = pltpu.SemaphoreType.DMA
    many, some = dma((bands,)), dma((team,))
    return pl.pallas_call(
        functools.partial(ace_kernel, bands, groups),
        name="ace",
        out_shape=(
            jax.ShapeDtypeStruct((own, width), BF16),
            jax.ShapeDtypeStruct((bown, width), BF16),
        ),
        in_specs=[hbm, hbm, hbm],
        out_specs=(hbm, hbm),
        scratch_shapes=[
            pltpu.VMEM((1, width), F32),
            pltpu.VMEM((n, cols), BF16),
            pltpu.VMEM((n, cols), BF16),
            pltpu.VMEM((n, cols), BF16),
            pltpu.VMEM((n, cols), BF16),
            pltpu.VMEM((n, n), F32),
            pltpu.VMEM((n, n), F32),
            pltpu.VMEM((n, n), BF16),
            pltpu.VMEM((n, n), BF16),
            pltpu.VMEM((n2, n2), BF16),
            pltpu.VMEM((TILE, 2 * TILE), F32),
            pltpu.VMEM((TILE, TILE), F32),
            pltpu.VMEM((n, cols), BF16),
            pltpu.VMEM((n, cols), BF16),
            pltpu.VMEM((nblk, cols), BF16),
            pltpu.VMEM((nblk, cols), F32),
            pltpu.VMEM((nblk, cols), BF16),
            pltpu.VMEM((nblk // 2, cols), BF16),
            pltpu.VMEM((nblk // 2, n), F32),
            dma((6,)), some, some, some, some, some, some, dma((team, 2)), dma((team, 2)),
            many, many, dma((1,)), dma((1,)), dma((1,)),
            many, many, many, many,
        ]
        + reduce_scratch(padded(tiles * (tiles + 1) // 2 * TILE, team), team, bands, levels, 2)
        + reduce_scratch(padded(tiles * tiles * TILE, bands), bands, bands, levels, 1)
        + reduce_scratch(2 * n, bands, bands, levels, 1),
        compiler_params=pltpu.CompilerParams(
            collective_id=0, has_side_effects=True, vmem_limit_bytes=56 * 2**20),
    )(orbitals, kernel.reshape(1, width), block_vectors)


def solution(mesh):
    placed = (P(("img", "band"), "ga"), P("ga"), P(("img", "band"), "ga"))
    return jax.shard_map(
        shards,
        mesh=mesh,
        in_specs=placed,
        out_specs=(P(("img", "band"), "ga"), P(("img", "band"), "ga")),
        check_vma=False,
    )
```

```python
import functools

import jax
import jax.numpy as jnp
from jax import lax
from jax.experimental import pallas as pl
from jax.experimental.pallas import tpu as pltpu
from jax.sharding import PartitionSpec as P

MESH = pl.DeviceIdType.MESH
F32 = jnp.float32
BF16 = jnp.bfloat16
TILE = 128
LANES = 128


def remote(src, dst, send_sem, recv_sem, where):
    return pltpu.make_async_remote_copy(
        src_ref=src, dst_ref=dst, send_sem=send_sem, recv_sem=recv_sem,
        device_id=where, device_id_type=MESH,
    )


def greet(places):
    barrier = pltpu.get_barrier_semaphore()
    for place in places:
        pl.semaphore_signal(barrier, inc=1, device_id=place, device_id_type=MESH)
    pl.semaphore_wait(barrier, len(places))


def dot(a, b, dims):
    return lax.dot_general(a, b, (dims, ((), ())), preferred_element_type=F32)


class Place:
    def __init__(self, bands, groups):
        self.bands = bands
        self.me = lax.axis_index("band")
        self.team = bands // 2
        self.half = self.me // self.team
        self.rank = lax.rem(self.me, self.team)
        ga = lax.axis_index("ga")
        self.core = lax.rem(ga, 2)
        self.row = lax.rem(ga // 2, 2)
        self.partner = {"ga": ga + 1 - 2 * self.core}
        self.across = {"ga": ga + 2 - 4 * self.row}
        self.peer = [lax.rem(self.me + d, bands) for d in range(bands)]
        self.far = sorted(range(1, bands), key=lambda d: -min(d, bands - d))
        self.near = self.far[::-1]
        self.bits = []
        stride = 4
        while stride < groups:
            self.bits.append({"ga": ga + stride * (1 - 2 * lax.rem(ga // stride, 2))})
            stride *= 2

    def band(self, d):
        return {"band": self.peer[d]}

    def mate(self, j):
        return lax.rem(self.rank + j, self.team)

    def rival(self, t):
        return (1 - self.half) * (self.team + t) + self.half * (self.team - 1 - t)

    def everyone(self):
        return [self.band(d) for d in range(1, self.bands)] + [self.partner, self.across] + self.bits


def span(index, size, offset=0, stride=None):
    return pl.ds(pl.multiple_of(offset + index * (stride or size), 16), size)


def reduce_scratch(rows, parts, bands, levels, sides):
    h1, h2 = rows // 2, rows // 4
    h3 = h2 // parts
    dma = pltpu.SemaphoreType.DMA
    shapes = [
        ((rows, TILE), F32), ((rows, TILE), BF16), ((h1, TILE), BF16),
        ((h1, TILE), F32), ((h1, TILE), BF16), ((h2, TILE), BF16),
        ((h2, TILE), F32), ((h2, TILE), BF16), ((parts, h3, TILE), BF16),
        ((levels, h3, TILE), BF16), ((levels, h3, TILE), BF16), ((sides * rows, TILE), BF16),
    ]
    return [pltpu.VMEM(*shape) for shape in shapes] + [
        dma((4,)), dma((1,)), dma((1,)), dma((levels,)), dma((levels,)),
        dma((bands,)), dma((bands,)), dma((1,)), dma((1,)),
        dma((1,)), dma((1,)),
    ]


SCRATCH = 23


class Reduce:
    def __init__(self, at, scratch, by_team):
        self.at = at
        (self.p32, self.p16, self.rx1, self.a32, self.a16, self.rx2, self.b32, self.b16, self.rx3,
         self.out_x, self.rx_x, self.allg, self.one, self.z_s, self.z_r, self.x_s, self.x_r,
         self.g_s, self.g_r, self.y_s, self.y_r, self.f_s, self.f_r) = scratch
        self.rows = self.p32.shape[0]
        self.h1, self.h2, self.h3 = self.rx1.shape[0], self.rx2.shape[0], self.rx3.shape[1]
        self.by_team = by_team
        if by_team:
            self.mine = at.rank
            self.parts = [(j, at.mate(j), {"band": at.half * at.team + at.mate(j)})
                          for j in range(1, at.team)]
        else:
            self.mine = at.me
            self.parts = [(d, at.peer[d], at.band(d)) for d in at.far]

    def put(self, row, value):
        size = value.shape[0]
        self.p32[row:row + size, :] = value
        self.p16[row:row + size, :] = value.astype(BF16)

    def pad(self, row):
        size = self.rows - row
        if size:
            self.put(row, jnp.zeros((size, TILE), F32))

    def to_partner(self):
        at = self.at
        return remote(self.p16.at[span(1 - at.core, self.h1)], self.rx1,
                      self.one.at[0], self.one.at[1], at.partner)

    def to_across(self):
        at = self.at
        return remote(self.a16.at[span(1 - at.row, self.h2)], self.rx2,
                      self.one.at[2], self.one.at[3], at.across)

    def to_parts(self):
        return [remote(self.b16.at[span(index, self.h3)], self.rx3.at[slot],
                       self.z_s.at[0], self.z_r.at[0], where)
                for slot, index, where in self.parts]

    def piece(self, d, row):
        at = self.at
        source = lax.rem(at.me + at.bands - d, at.bands)
        offset = at.core * self.h1 + row * self.h2
        if self.by_team:
            offset = offset + (source // at.team) * self.rows
            source = lax.rem(source, at.team)
        return span(source, self.h3, offset)

    def gather(self, d):
        own = self.allg.at[self.piece(0, self.at.row)]
        return remote(own, own, self.g_s.at[d], self.g_r.at[d], self.at.band(d))

    def side(self, d):
        there = self.allg.at[self.piece(d, self.at.row)]
        return remote(there, there, self.y_s.at[0], self.y_r.at[0], self.at.across)

    def last(self, d, other):
        row = 1 - self.at.row if other else self.at.row
        there = self.allg.at[self.piece(d, row)]
        return remote(there, there, self.f_s.at[0], self.f_r.at[0], self.at.partner)

    def s1(self):
        self.to_partner().start()

    def s2(self):
        self.to_partner().wait()
        self.a32[...] = self.p32[span(self.at.core, self.h1), :] + self.rx1[...].astype(F32)
        self.a16[...] = self.a32[...].astype(BF16)
        self.to_across().start()

    def s3(self):
        self.to_across().wait()
        self.b32[...] = self.a32[span(self.at.row, self.h2), :] + self.rx2[...].astype(F32)
        self.b16[...] = self.b32[...].astype(BF16)
        for copy in self.to_parts():
            copy.start()

    def s4(self):
        at = self.at
        whole = self.rx3.at[0:len(self.parts)]
        remote(whole, whole, self.z_s.at[0], self.z_r.at[0], self.parts[0][2]).wait()
        total = self.b32[span(self.mine, self.h3), :]
        for slot, _, _ in self.parts:
            total = total + self.rx3[slot].astype(F32)
        for i, place in enumerate(at.bits):
            self.out_x[i] = total.astype(BF16)
            copy = remote(self.out_x.at[i], self.rx_x.at[i], self.x_s.at[i], self.x_r.at[i], place)
            copy.start()
            copy.wait()
            total = self.out_x[i].astype(F32) + self.rx_x[i].astype(F32)
        self.allg[self.piece(0, at.row), :] = total.astype(BF16)
        for d in at.far:
            self.gather(d).start()
        self.side(0).start()
        self.last(0, 0).start()

    def s5(self):
        for d in self.at.near:
            self.gather(d).wait()
            self.side(d).start()
            self.last(d, 0).start()

    def s6(self):
        whole = self.allg.at[0:self.at.bands * self.h3]
        remote(whole, whole, self.y_s.at[0], self.y_r.at[0], self.at.across).wait()
        for d in [0] + self.at.near:
            self.last(d, 1).start()

    def s7(self):
        whole = self.allg.at[0:2 * self.at.bands * self.h3]
        remote(whole, whole, self.f_s.at[0], self.f_r.at[0], self.at.partner).wait()


def split(a):
    high = a.astype(BF16)
    return high, (a - high.astype(F32)).astype(BF16)


def product3(a, b, dims):
    (ah, al), (bh, bl) = split(a), split(b)
    return dot(ah, bh, dims) + (dot(ah, bl, dims) + dot(al, bh, dims))


def identity(rows):
    shape = (rows, rows)
    return (lax.broadcasted_iota(jnp.int32, shape, 0)
            == lax.broadcasted_iota(jnp.int32, shape, 1)).astype(F32)


def factor_tile(d_ref, t_ref, hooks):
    G, SUB, BLK = 32, 8, 16
    H, K = G // SUB, BLK // SUB
    sub = lax.broadcasted_iota(jnp.int32, (SUB, TILE), 0)

    def spread(block, i):
        return jnp.broadcast_to(block[i:i + 1, :], (SUB, TILE))

    def lane(block, c):
        where = jnp.full((SUB, TILE), c, jnp.int32)
        return jnp.take_along_axis(block, where, axis=1, mode="promise_in_bounds")

    def step(g, carry):
        start = g * G if isinstance(g, int) else pl.multiple_of(g * G, G)
        lefts = [d_ref[pl.ds(start + h * SUB, SUB), 0:TILE] for h in range(H)]
        rights = [d_ref[pl.ds(start + h * SUB, SUB), TILE:2 * TILE] for h in range(H)]
        us, vs = [None] * H, [None] * H
        for b in range(G // BLK):
            h0 = b * K
            cols = [{h: lane(lefts[h], start + (b * BLK + c)) for h in range(h0 + c // SUB, H)}
                    for c in range(BLK)]
            pivot = spread(cols[0][h0], 0)
            for j in range(BLK):
                k, i = h0 + j // SUB, j % SUB
                r = lax.rsqrt(pivot)
                low = {c: spread(cols[j][h0 + c // SUB], c % SUB) for c in range(j + 1, BLK)}
                if j + 1 < BLK:
                    low[j + 1] = low[j + 1] * r
                    pivot = spread(cols[j + 1][h0 + (j + 1) // SUB], (j + 1) % SUB) - low[j + 1] * low[j + 1]
                for h in range(k, H):
                    cols[j][h] = cols[j][h] * r
                u, v = spread(lefts[k], i) * r, spread(rights[k], i) * r
                us[k] = u if i == 0 else jnp.where(sub == i, u, us[k])
                vs[k] = v if i == 0 else jnp.where(sub == i, v, vs[k])
                for c in range(j + 1, BLK):
                    scaled = low[c] if c == j + 1 else low[c] * r
                    for h in range(h0 + c // SUB, H):
                        cols[c][h] = cols[c][h] - cols[j][h] * scaled
                for h in range(k if i < SUB - 1 else k + 1, H):
                    lefts[h] = lefts[h] - cols[j][h] * u
                    rights[h] = rights[h] - cols[j][h] * v
        u_all = jnp.concatenate(us, axis=0)
        v_all = jnp.concatenate(vs, axis=0)
        t_ref[pl.ds(start, G), :] = v_all
        if isinstance(g, int):
            for stage in hooks[g]:
                stage()
            return carry
        both = jnp.concatenate([u_all, v_all], axis=1)
        high = both.astype(BF16).astype(F32)
        low = both - high
        lhs = jnp.concatenate([high[:, :TILE], high[:, :TILE], low[:, :TILE]], axis=0)
        rhs = jnp.concatenate([high, low, high], axis=0)
        d_ref[...] -= dot(lhs.astype(BF16), rhs.astype(BF16), ((0,), (0,)))
        for k, stages in enumerate(hooks[:-1]):
            if stages:
                @pl.when(g == k)
                def _():
                    for stage in stages:
                        stage()
        return carry

    lax.fori_loop(0, TILE // G - 1, step, 0)
    step(TILE // G - 1, 0)


def ace_kernel(bands, groups, orb, kern_in, blk, ace, exch, kern, full, extra, w, wx, a, rest, x16, xlow, mba,
               d_ref, t_ref, proj, proj2, bfull, acc, applied, applied2, back, loc, m_s, m_r, n_s, n_r, c_s, c_r,
               d_s, d_r, b_s, b_r, p_s, p_r, t_s, e_s, e_r, f_s, f_r, *scratch):
    at = Place(bands, groups)
    me, team = at.me, at.team
    own, bown = ace.shape[0], exch.shape[0]
    cols = w.shape[1]
    n, nblk = own * bands, bown * bands
    n2 = n // 2
    scale = 1.0 / (ace.shape[1] * groups)
    inner = Reduce(at, scratch[:SCRATCH], True)
    cross = Reduce(at, scratch[SCRATCH:2 * SCRATCH], False)
    couple = Reduce(at, scratch[2 * SCRATCH:], False)
    greet(at.everyone())

    def chunk(index):
        return pl.ds(pl.multiple_of(index * cols, TILE), cols)

    def twin(index):
        return chunk(lax.rem(index + team, bands))

    mine = full.at[span(me, own)]
    also = extra.at[span(me, own)]
    bmine = bfull.at[span(me, bown)]

    def kept():
        return [pltpu.make_async_copy(orb.at[:, chunk(me)], mine, loc.at[0]),
                pltpu.make_async_copy(orb.at[:, twin(me)], also, loc.at[1]),
                pltpu.make_async_copy(kern_in, kern, loc.at[5])]

    def to_mates():
        copies = []
        for j in range(1, team):
            p = at.half * team + at.mate(j)
            copies.append(remote(orb.at[:, chunk(p)], mine, m_s.at[j], m_r.at[j], {"band": p}))
            copies.append(remote(orb.at[:, twin(p)], also, n_s.at[j], n_r.at[j], {"band": p}))
        return copies

    def to_rival(t, sender):
        p = at.rival(t)
        return remote(orb.at[:, chunk(p)], mine, c_s.at[t], c_r.at[sender], {"band": p})

    parts = [(0, cols // 2 // LANES * LANES), (cols // 2 // LANES * LANES, cols)]
    parts = [part for part in parts if part[0] < part[1]]

    def twin_rival(t, sender, lo, hi):
        p = at.rival(t)
        first = pl.multiple_of(lax.rem(p + team, bands) * cols + lo, TILE)
        k = 0 if hi <= parts[0][1] else 1
        return remote(orb.at[:, pl.ds(first, hi - lo)], extra.at[span(me, own), lo:hi],
                      d_s.at[t, k], d_r.at[sender, k], {"band": p})

    slices = [(t, lo) for t in reversed(range(team)) for lo in range(0, cols, LANES)]
    left = {True: list(slices), False: list(slices)}
    near = at.rank >= team // 2

    def upward(count, first=True):
        batch, left[first][:] = left[first][:count], left[first][count:]

        def go():
            @pl.when((at.half == 0) & (near if first else ~near))
            def _():
                for t, lo in batch:
                    twin_rival(t, at.rank, lo, lo + LANES).start()
        return go

    def block(slot, p, sender):
        return remote(blk.at[:, chunk(p)], bmine, b_s.at[slot], b_r.at[sender], {"band": p})

    def block_rival(t):
        return lambda: block(t, at.rival(t), me).start()

    def block_mates():
        for j in range(1, team):
            block(team + j, at.half * team + at.mate(j), me).start()

    def bkept():
        return pltpu.make_async_copy(blk.at[:, chunk(me)], bmine, loc.at[2])

    for copy in to_mates():
        copy.start()
    for t in range(team):
        to_rival(t, at.rank).start()
    for copy in kept():
        copy.start()
    bkept().start()

    def weigh(rows, columns):
        return (-(rows.astype(F32) * kern[:, columns])).astype(BF16)

    for copy in kept() + to_mates():
        copy.wait()
    band = span(at.half, n2)
    w[band, :] = weigh(full[band, :], chunk(me))
    wx[band, :] = weigh(extra[band, :], twin(me))
    row = 0
    for s in range(0, n2, TILE):
        e = s + TILE
        product = (dot(w[span(at.half, TILE, s, n2), :], full[span(at.half, e, 0, n2), :],
                       ((1,), (1,)))
                   + dot(wx[span(at.half, TILE, s, n2), :], extra[span(at.half, e, 0, n2), :],
                         ((1,), (1,))))
        for c in range(0, e, TILE):
            inner.put(row, product[:, c:c + TILE])
            row += TILE
    inner.pad(row)
    inner.s1()
    inner.s2()
    inner.s3()
    for t in range(team):
        to_rival(t, t).wait_recv()
    other = span(1 - at.half, n2)
    w[other, :] = weigh(full[other, :], chunk(me))
    row = 0
    for s in range(n2, n, TILE):
        product = dot(w[s:s + TILE, :], full[0:n2, :], ((1,), (1,)))
        for c in range(0, n2, TILE):
            cross.put(row, product[:, c:c + TILE])
            row += TILE
    cross.pad(row)
    cross.s1()
    inner.s4()
    for t in range(team - 1):
        block_rival(t)()
    cross.s2()
    inner.s5()
    cross.s3()
    block_rival(team - 1)()
    block_mates()
    inner.s6()
    inner.s7()
    row = 0
    for base in (0, n2):
        for s in range(base, base + n2, TILE):
            for c in range(base, s + TILE, TILE):
                a[s:s + TILE, c:c + TILE] = inner.allg[row:row + TILE, :].astype(F32) * -scale
                row += TILE
        row = inner.rows
    rest[...] = identity(n)
    x16[...] = jnp.zeros_like(x16)
    xlow[...] = jnp.zeros_like(xlow)

    def couple_start():
        bkept().wait()
        for d in range(1, bands):
            block(d, at.peer[d], at.peer[d]).wait_recv()
        half = nblk // 2
        for h in range(2):
            couple.put(h * n, dot(w[...], bfull[h * half:(h + 1) * half, :], ((1,), (1,))))
        couple.s1()

    cuts = sorted(set(range(0, n, TILE)) | set(range(0, n, own)) | {n})
    pieces = list(enumerate(zip(cuts[:-1], cuts[1:])))

    def piece(q, r0, r1, source, target, other):
        lo = r0 % own
        if other:
            return strip(q, r0, r1, source, target, 0, 0, cols)
        return remote(proj.at[r0:r1], ace.at[lo:lo + r1 - r0, chunk(source)],
                      p_s.at[0], p_r.at[0], {"band": target})

    def stay(q, r0, r1, other):
        lo = r0 % own
        if other:
            return strip_stay(q, r0, r1, 0, 0, cols)
        return pltpu.make_async_copy(
            proj.at[r0:r1], ace.at[lo:lo + r1 - r0, chunk(me)], t_s.at[0])

    def some(source, c0, c1):
        first = lax.rem(source + team, bands) * cols + c0
        return pl.ds(pl.multiple_of(first, TILE), c1 - c0)

    def strip(q, r0, r1, source, target, k, c0, c1):
        lo = r0 % own
        return remote(proj2.at[r0:r1, c0:c1], ace.at[lo:lo + r1 - r0, some(source, c0, c1)],
                      p_s.at[0], p_r.at[0], {"band": target})

    def strip_stay(q, r0, r1, k, c0, c1):
        lo = r0 % own
        return pltpu.make_async_copy(
            proj2.at[r0:r1, c0:c1], ace.at[lo:lo + r1 - r0, some(me, c0, c1)], t_s.at[0])

    def deliver(lo, hi, other):
        for q, (r0, r1) in pieces:
            if lo <= r0 < hi:
                owner = r0 // own

                @pl.when((me != owner) & (at.half == owner // team))
                def _():
                    piece(q, r0, r1, me, owner, other).start()

                @pl.when(me == owner)
                def _():
                    stay(q, r0, r1, other).start()

    def project(lo, hi, c0, c1):
        proj2[lo:hi, c0:c1] = (dot(x16[lo:hi, 0:hi], wx[0:hi, c0:c1], ((1,), (0,)))
                               + dot(xlow[lo:hi, 0:hi], wx[0:hi, c0:c1], ((1,), (0,)))).astype(BF16)

    def spare():
        @pl.when(at.half == 0)
        def _():
            project(0, n2, 0, cols)

        deliver(0, n2, 1)

    tiles = n2 // TILE
    hooks = [[[] for _ in range(4)] for _ in range(2 * tiles)]

    def at_hook(k, g, *stages):
        hooks[k][g] += stages

    at_hook(0, 1, cross.s4, upward(2))
    at_hook(0, 3, upward(1))
    at_hook(tiles - 2, 0, couple_start)
    at_hook(tiles - 2, 1, cross.s5)
    at_hook(tiles - 2, 2, couple.s2)
    at_hook(tiles - 2, 3, upward(1), upward(1, False))
    at_hook(tiles - 1, 0, upward(1), upward(1, False))
    at_hook(tiles - 1, 1, upward(1))
    at_hook(tiles - 1, 1, cross.s6)
    closing = upward(3)
    at_hook(tiles, 1, couple.s4, lambda: deliver(0, n2 - TILE, 0), upward(len(slices)))
    at_hook(tiles + 1, 0, upward(len(slices), False), lambda: deliver(n2 - TILE, n2, 0))
    at_hook(tiles + 1, 2, couple.s5, spare)
    at_hook(tiles + 2, 1, couple.s6)
    at_hook(tiles + 2, 3, couple.s7)

    def attach(lo, hi):
        half = nblk // 2
        for h in range(2):
            part = allg_dot(lo, hi, h) * scale
            update = dot(part.astype(BF16), proj[lo:hi, :], ((0,), (0,)))
            if lo == 0:
                acc[h * half:(h + 1) * half, :] = update
            else:
                acc[h * half:(h + 1) * half, :] += update

    def allg_dot(lo, hi, h):
        return dot(x16[lo:hi, 0:hi], couple.allg[h * n:h * n + hi, :], ((1,), (0,)))

    for k, s in enumerate(range(0, n, TILE)):
        e = s + TILE
        top = n2 if s < n2 else n
        d_ref[:, 0:TILE] = a[s:e, s:e]
        d_ref[:, TILE:] = identity(TILE)
        factor_tile(d_ref, t_ref, hooks[k])
        tile = t_ref[...]
        rows = product3(tile, rest[s:e, 0:e], ((1,), (0,)))
        high, low = split(rows)
        x16[s:e, 0:e] = high
        xlow[s:e, 0:e] = low
        proj[s:e, :] = (dot(high, w[0:e, :], ((1,), (0,)))
                        + dot(low, w[0:e, :], ((1,), (0,)))).astype(BF16)
        if s >= n2:
            deliver(s, e, 0)
        if e < top:
            panel = product3(a[e:top, s:e], tile, ((1,), (1,)))
            for c in range(e, top, TILE):
                a[c:top, c:c + TILE] -= product3(panel[c - e:], panel[c - e:c - s], ((1,), (1,)))
            rest[e:top, 0:e] -= product3(panel, rows, ((1,), (0,)))
        if e == n2:
            cross.s7()
            row = 0
            for r in range(0, n2, TILE):
                for c in range(0, n2, TILE):
                    mba[r:r + TILE, c:c + TILE] = cross.allg[row:row + TILE, :]
                    row += TILE
            both = (((1,), (1,)))
            below = (dot(mba[...], x16[0:n2, 0:n2], both) + dot(mba[...], xlow[0:n2, 0:n2], both)) * -scale
            bh, bl = split(below)
            for c in range(0, n2, TILE):
                d = c + TILE
                a[n2 + c:n, n2 + c:n2 + d] -= (
                    dot(bh[c:], bh[c:d], both) + (dot(bh[c:], bl[c:d], both) + dot(bl[c:], bh[c:d], both)))
            over = ((1,), (0,))
            xh = x16[0:n2, 0:n2]
            couple.s3()
            closing()
            rest[n2:, 0:n2] = -(dot(bh, xh, over) + (dot(bh, xlow[0:n2, 0:n2], over) + dot(bl, xh, over)))
    attach(0, n)
    applied[...] = (-acc[...]).astype(BF16)

    def out(slot, p, sender):
        return remote(applied.at[span(p, bown)], exch.at[:, chunk(sender)],
                      e_s.at[slot], e_r.at[sender], {"band": p})

    def out2(slot, p, sender):
        return remote(applied2.at[span(lax.rem(p, team), bown)], exch.at[:, twin(sender)],
                      f_s.at[slot], f_r.at[sender], {"band": p})

    def held():
        return pltpu.make_async_copy(applied.at[span(me, bown)], exch.at[:, chunk(me)], loc.at[3])

    def held2():
        return pltpu.make_async_copy(applied2.at[span(at.rank, bown)], exch.at[:, twin(me)], loc.at[4])

    mates = [at.half * team + at.mate(j) for j in range(1, team)]

    @pl.when(at.half == 1)
    def _():
        for t in range(team):
            out(t, at.rival(t), me).start()

    for j, p in enumerate(mates):
        out(team + j, p, me).start()
    held().start()

    @pl.when(at.half == 1)
    def _():
        turned = ((0,), (0,))
        part = dot(x16[...], couple.allg[n:2 * n, :], ((1,), (0,))) * -scale
        ph, pq = split(part)
        back[...] = (dot(ph, x16[...], turned)
                     + (dot(ph, xlow[...], turned) + dot(pq, x16[...], turned)))

    @pl.when(at.half == 1)
    def _():
        bh, bl = split(back[...])
        forth = ((1,), (0,))
        for k, (c0, c1) in enumerate(parts):
            for t in range(team):
                twin_rival(t, t, c0, c1).wait_recv()
            wx[0:n2, c0:c1] = (-(extra[0:n2, c0:c1].astype(F32) * kern[:, some(me, c0, c1)])).astype(BF16)
            project(n2, n, c0, c1)
            for q, (r0, r1) in pieces:
                if r0 >= n2:
                    owner = r0 // own

                    @pl.when(me != owner)
                    def _():
                        strip(q, r0, r1, me, owner, k, c0, c1).start()

                    @pl.when(me == owner)
                    def _():
                        strip_stay(q, r0, r1, k, c0, c1).start()

            applied2[:, c0:c1] = (dot(bh, wx[:, c0:c1], forth) + dot(bl, wx[:, c0:c1], forth)).astype(BF16)
        for j, p in enumerate(mates):
            out2(j, p, me).start()
        held2().start()

    for t in range(team):
        to_rival(t, t).wait_send()
        block(t, me, me).wait_send()
    for j in range(1, team):
        block(team + j, me, me).wait_send()

    @pl.when(at.half == 0)
    def _():
        for t in range(team):
            for c0, c1 in parts:
                twin_rival(t, t, c0, c1).wait_send()

    everything = ace.at[:, 0:2 * cols * (team - 1)]
    remote(everything, everything, p_s.at[0], p_r.at[0], {"band": mates[0]}).wait()
    local = ace.at[:, 0:2 * cols]
    pltpu.make_async_copy(local, local, t_s.at[0]).wait()
    for j, p in enumerate(mates):
        out(team + j, p, p).wait()
    held().wait()

    @pl.when(at.half == 1)
    def _():
        for t in range(team):
            out(t, at.rival(t), me).wait_send()
        for j, p in enumerate(mates):
            out2(j, p, p).wait()
        held2().wait()

    @pl.when(at.half == 0)
    def _():
        for t in range(team):
            out(t, me, at.rival(t)).wait_recv()


def shards(orbitals, kernel, block_vectors):
    groups, bands = lax.axis_size("ga"), lax.axis_size("band")
    own, width = orbitals.shape
    bown = block_vectors.shape[0]
    cols = width // bands
    n, nblk = own * bands, bown * bands
    n2, team = n // 2, bands // 2
    levels = max(groups.bit_length() - 3, 1)
    tiles = n2 // TILE

    def padded(rows, parts):
        unit = 4 * parts * 16
        return -(-rows // unit) * unit

    hbm = pl.BlockSpec(memory_space=pl.ANY)
    dma = pltpu.SemaphoreType.DMA
    many, some = dma((bands,)), dma((team,))
    return pl.pallas_call(
        functools.partial(ace_kernel, bands, groups),
        name="ace",
        out_shape=(
            jax.ShapeDtypeStruct((own, width), BF16),
            jax.ShapeDtypeStruct((bown, width), BF16),
        ),
        in_specs=[hbm, hbm, hbm],
        out_specs=(hbm, hbm),
        scratch_shapes=[
            pltpu.VMEM((1, width), F32),
            pltpu.VMEM((n, cols), BF16),
            pltpu.VMEM((n, cols), BF16),
            pltpu.VMEM((n, cols), BF16),
            pltpu.VMEM((n, cols), BF16),
            pltpu.VMEM((n, n), F32),
            pltpu.VMEM((n, n), F32),
            pltpu.VMEM((n, n), BF16),
            pltpu.VMEM((n, n), BF16),
            pltpu.VMEM((n2, n2), BF16),
            pltpu.VMEM((TILE, 2 * TILE), F32),
            pltpu.VMEM((TILE, TILE), F32),
            pltpu.VMEM((n, cols), BF16),
            pltpu.VMEM((n, cols), BF16),
            pltpu.VMEM((nblk, cols), BF16),
            pltpu.VMEM((nblk, cols), F32),
            pltpu.VMEM((nblk, cols), BF16),
            pltpu.VMEM((nblk // 2, cols), BF16),
            pltpu.VMEM((nblk // 2, n), F32),
            dma((6,)), some, some, some, some, some, some, dma((team, 2)), dma((team, 2)),
            many, many, dma((1,)), dma((1,)), dma((1,)),
            many, many, many, many,
        ]
        + reduce_scratch(padded(tiles * (tiles + 1) // 2 * TILE, team), team, bands, levels, 2)
        + reduce_scratch(padded(tiles * tiles * TILE, bands), bands, bands, levels, 1)
        + reduce_scratch(2 * n, bands, bands, levels, 1),
        compiler_params=pltpu.CompilerParams(
            collective_id=0, has_side_effects=True, vmem_limit_bytes=56 * 2**20),
    )(orbitals, kernel.reshape(1, width), block_vectors)


def solution(mesh):
    placed = (P(("img", "band"), "ga"), P("ga"), P(("img", "band"), "ga"))
    return jax.shard_map(
        shards,
        mesh=mesh,
        in_specs=placed,
        out_specs=(P(("img", "band"), "ga"), P(("img", "band"), "ga")),
        check_vma=False,
    )
```
